256 devices in a mesh: grp: 2 (over z), gx: 64 (over x, y), gz: 2 (over core).
Axes of the slice: x: 8, y: 8, z: 2, core: 2. Of those that a mesh axis runs over, the one named last changes fastest.
The devices are a block of a 8x8x16 slice.
Arguments:
- electric: float32 [4096, 8192], P(('grp', 'gx'), 'gz'), parts along dimension 0, may hold values from -6 to 6
- magnetic_x: float32 [4096, 8192], P(('grp', 'gx'), 'gz'), parts along dimension 0, may hold values from -6 to 6
- magnetic_z: float32 [4096, 8192], P(('grp', 'gx'), 'gz'), parts along dimension 0, may hold values from -6 to 6
- index_map: int32 [4, 64, 8192], P(None, None, 'gz'), may hold values from 0 to 3
- period_seq: int32 [66], P('grp'), parts along dimension 0, may hold values from 0 to 3
- eps_table: float32 [4], replicated, may hold values from 1 to 12.25
- shifts: int32 [8], P('grp'), parts along dimension 0, may hold values from 0 to 4, as said below
Outputs:
- electric_out: float32 [4096, 8192], P(('grp', 'gx'), 'gz'), parts along dimension 0
- magnetic_x_out: float32 [4096, 8192], P(('grp', 'gx'), 'gz'), parts along dimension 0
- magnetic_z_out: float32 [4096, 8192], P(('grp', 'gx'), 'gz'), parts along dimension 0
The draws below stay inside these ranges and needn't reach their ends.
There are 2 independent parts, one for each index of `grp`. The reference program is written for one: setup_inputs(seed, part) draws one part's arguments, and reference() takes and returns one part's arrays. A program takes and returns all parts, laid end to end along the dimension named above; an argument that names none is the same for every part. Nothing has to cross between parts.
Inputs may be any that keep to these rules, and one draw needn't show every extreme that they name: `shifts`: every entry is at most 4, and some entry equals 4.
All inputs are finite; a program needn't handle non-finite values.
Results may differ from the reference program's by a relative error of at most 0.00016.
Values sent between devices are 32-bit elements; how exact they have to be, the bound alone decides.
A program may use at most 64 MiB of HBM per device.

```python
import math
import jax
import jax.numpy as jnp
from jax import lax

ITERS = 4
SMAX = 4
PER = 64
TYPES = 4
LEVELS = 4
NX = 2048
NZ = 8192
NP = 33


def draw_shifts(key, part):
    values = jax.random.randint(key, (ITERS,), 0, SMAX + 1, dtype=jnp.int32)
    where_most = jax.random.randint(jax.random.fold_in(key, 7), (), 0, ITERS, dtype=jnp.int32)
    return values.at[where_most].set(SMAX)


def plant(result, key, smallest, top_value):
    dims = result.shape
    spot = [jax.random.randint(jax.random.fold_in(key, axis), (), 0, dims[axis]) for axis in range(len(dims))]
    result = result.at[tuple(spot)].set(smallest)
    longest = dims.index(max(dims))
    spot[longest] = (spot[longest] + 1) % dims[longest]
    return result.at[tuple(spot)].set(top_value)


def block_levels(rng, shape, shards, low, top_value):
    gain = 1.0
    for axis_at, parts in shards:
        heights = jax.random.uniform(jax.random.fold_in(jax.random.fold_in(rng, 6), axis_at), (parts,), jnp.float32, low / len(shards), top_value / len(shards))
        gain = gain * jnp.repeat(jnp.exp(heights), shape[axis_at] // parts).reshape((-1,) + (1,) * (len(shape) - 1 - axis_at))
    return gain


def noise(rng, extent, deviation, limit, cuts=(), kind=jnp.bfloat16):
    result = deviation * jax.random.normal(rng, extent, jnp.float32)
    if cuts:
        result = result * block_levels(rng, extent, cuts, -0.22, 0.18)
    return jnp.clip(result, -limit, limit).astype(kind)


def setup_inputs(seed: int = 0, part: int = 0) -> dict:
    key_list = jax.random.split(jax.random.key(seed), 8)
    part_keys = jax.random.split(jax.random.fold_in(key_list[7], part), 8)
    electric = noise(part_keys[0], (NX, NZ), 1.0, 6.0, ((0, 64), (1, 2)), jnp.float32)
    magnetic_x = noise(part_keys[1], (NX, NZ), 1.0, 6.0, ((0, 64), (1, 2)), jnp.float32)
    magnetic_z = noise(part_keys[2], (NX, NZ), 1.0, 6.0, ((0, 64), (1, 2)), jnp.float32)
    index_map = plant(jax.random.randint(key_list[3], (TYPES, PER, NZ), 0, LEVELS), jax.random.fold_in(key_list[3], 1), 0, LEVELS - 1).astype(jnp.int32)
    period_seq = plant(jax.random.randint(part_keys[4], (NP,), 0, TYPES), jax.random.fold_in(part_keys[4], 1), 0, TYPES - 1).astype(jnp.int32)
    eps_table = jnp.clip(jnp.exp(jax.random.uniform(key_list[5], (LEVELS,), jnp.float32, math.log(1.0), math.log(12.25))), 1.0, 12.25)
    shifts = draw_shifts(jax.random.fold_in(jax.random.fold_in(key_list[7], part), 71), part)
    return dict(electric=electric, magnetic_x=magnetic_x, magnetic_z=magnetic_z, index_map=index_map, period_seq=period_seq, eps_table=eps_table, shifts=shifts)


def reference(electric, magnetic_x, magnetic_z, index_map, period_seq, eps_table, shifts):
    inverse = 1.0 / eps_table
    total_x, total_z = electric.shape
    offset = jnp.int32(0)
    tail = jnp.zeros((SMAX, total_z), electric.dtype)
    fields = [electric, magnetic_x, magnetic_z]
    for step in range(ITERS):
        moved = shifts[step].astype(jnp.int32)
        offset = offset + moved
        fields = [lax.dynamic_slice_in_dim(jnp.concatenate([item, tail], axis=0), moved, total_x, 0) for item in fields]
        columns = jnp.arange(total_x, dtype=jnp.int32) + offset
        design = period_seq[columns // PER]
        layers = jnp.arange(total_z, dtype=jnp.int32)
        levels = index_map[design[:, None], (columns % PER)[:, None], layers[None, :]]
        coeff = inverse[levels]
        field_e, field_hx, field_hz = fields
        zero_col = jnp.zeros((total_x, 1), field_e.dtype)
        zero_row = jnp.zeros((1, total_z), field_e.dtype)
        upper = jnp.concatenate([field_e[:, 1:], zero_col], axis=1)
        field_hx = field_hx + 0.6 * (upper - field_e)
        ahead = jnp.concatenate([field_e[1:], zero_row], axis=0)
        field_hz = field_hz - 0.6 * (ahead - field_e)
        lower = jnp.concatenate([zero_col, field_hx[:, :-1]], axis=1)
        behind = jnp.concatenate([zero_row, field_hz[:-1]], axis=0)
        field_e = field_e + 0.6 * coeff * ((field_hx - lower) - (field_hz - behind))
        fields = [field_e, field_hx, field_hz]
    return fields[0], fields[1], fields[2]
```

```python
import functools

import jax
import jax.numpy as jnp
from jax import lax
from jax.experimental import pallas as pl
from jax.experimental.pallas import tpu as pltpu
from jax.sharding import PartitionSpec as P

ITERS = 4
SMAX = 4
COURANT = 0.6
MESH = pl.DeviceIdType.MESH

LANE = 128
PAD = 5
CHUNK = 4
REACH = ITERS * SMAX
EARLY = 2


def kernel(
    rows,
    own,
    span,
    shifts_ref,
    seq_ref,
    eps_ref,
    e_in,
    hx_in,
    hz_in,
    map_in,
    e_out,
    hx_out,
    hz_out,
    e0,
    hx0,
    hz0,
    e1,
    hx1,
    hz1,
    e2,
    hx2,
    hz2,
    e3,
    hx3,
    hz3,
    e4,
    hx4,
    hz4,
    coeff,
    design_rows,
    edge_rows,
    bound_out,
    bound_in,
    local_sem,
    edge_send,
    edge_recv,
    send_sem,
    recv_sem,
    bound_send_sem,
    bound_recv_sem,
    relay_send,
    relay_recv,
):
    me = lax.axis_index("gx")
    core = lax.axis_index("gz")
    count = lax.axis_size("gx")
    left = lax.rem(me + count - 1, count)
    right = lax.rem(me + 1, count)
    total = rows + REACH
    bands = total // 8
    own_bands = rows // 8
    chunks = own // CHUNK
    cells = own * LANE
    is_last = me == count - 1

    to_left = {"gx": left}
    to_right = {"gx": right}
    to_partner = {"gz": 1 - core}

    ins = (e_in, hx_in, hz_in)
    state = ((e0, hx0, hz0), (e1, hx1, hz1), (e2, hx2, hz2), (e3, hx3, hz3), (e4, hx4, hz4))
    start = state[0]
    mine = pl.ds(PAD * LANE, cells)

    def at(tile):
        return pl.ds(pl.multiple_of(tile * LANE, LANE), LANE)

    phase = lax.rem(me * rows, span)
    high = lax.rem(me * rows + rows, span)
    loads = [
        pltpu.make_async_copy(ins[f], start[f].at[pl.ds(0, rows), mine], local_sem.at[f])
        for f in range(3)
    ]
    loads.append(
        pltpu.make_async_copy(
            map_in.at[:, pl.ds(pl.multiple_of(phase, 8), rows), :],
            design_rows.at[:, pl.ds(0, rows), :],
            local_sem.at[3],
        )
    )
    loads.append(
        pltpu.make_async_copy(
            map_in.at[:, pl.ds(pl.multiple_of(high, 8), REACH), :],
            design_rows.at[:, pl.ds(rows, REACH), :],
            local_sem.at[4],
        )
    )
    for load in loads:
        load.start()

    barrier = pltpu.get_barrier_semaphore()
    pl.semaphore_signal(barrier, inc=1, device_id=to_right, device_id_type=MESH)
    pl.semaphore_signal(barrier, inc=1, device_id=to_partner, device_id_type=MESH)
    pl.semaphore_wait(barrier, 2)

    edge = (1 - core) * (own - 1)
    halo = jnp.where(core == 1, PAD + own, PAD - 1)
    here = jnp.where(core == 0, PAD + own, PAD - 1)
    outside = jnp.where(core == 1, PAD + own, PAD - 1)

    def remote(src, dst, send, recv, target):
        return pltpu.make_async_remote_copy(
            src_ref=src, dst_ref=dst, send_sem=send, recv_sem=recv, device_id=target, device_id_type=MESH
        )

    def bulk(f, first, width, slot):
        source = pl.ds(pl.multiple_of(first * LANE, LANE), width * LANE)
        target = pl.ds(pl.multiple_of((first + PAD) * LANE, LANE), width * LANE)
        return remote(
            ins[f].at[pl.ds(0, REACH), source],
            start[f].at[pl.ds(rows, REACH), target],
            send_sem.at[f, slot],
            recv_sem.at[f, slot],
            to_left,
        )

    def chunk_copy(f, j):
        if isinstance(j, int) and j == chunks - 1:
            return bulk(f, core + j * CHUNK, CHUNK - 1, j)
        return bulk(f, core + j * CHUNK, CHUNK, j)

    edge_copies = [bulk(f, edge, 1, chunks) for f in range(3)]
    partner_copies = [
        remote(
            ins[f].at[:, at(edge)],
            start[f].at[pl.ds(0, rows), at(halo)],
            edge_send.at[f],
            edge_recv.at[f],
            to_partner,
        )
        for f in range(3)
    ]
    partner_copies.append(
        remote(
            map_in.at[:, pl.ds(pl.multiple_of(phase, 8), rows), at(edge)],
            edge_rows.at[:, pl.ds(0, rows), :],
            edge_send.at[3],
            edge_recv.at[3],
            to_partner,
        )
    )
    partner_copies.append(
        remote(
            map_in.at[:, pl.ds(pl.multiple_of(high, 8), REACH), at(edge)],
            edge_rows.at[:, pl.ds(rows, REACH), :],
            edge_send.at[4],
            edge_recv.at[4],
            to_partner,
        )
    )
    for copy in edge_copies:
        copy.start()
    for copy in partner_copies:
        copy.start()
    for j in range(EARLY):
        for f in range(3):
            chunk_copy(f, j).start()

    lane = lax.broadcasted_iota(jnp.int32, (8, LANE), 1)
    sub = lax.broadcasted_iota(jnp.int32, (8, LANE), 0)
    zero = jnp.zeros((8, LANE), jnp.float32)
    last_vec = jnp.full((8, LANE), me, jnp.int32) == count - 1
    offsets = []
    offset = jnp.int32(0)
    for step in range(ITERS):
        offset = offset + shifts_ref[step]
        offsets.append(offset)

    for f in range(3):
        for r in range(bands):
            start[f][pl.ds(8 * r, 8), at(outside)] = zero

    gains = [COURANT * (1.0 / jnp.full((8, LANE), eps_ref[k], jnp.float32)) for k in range(4)]
    period = me * rows // span
    next_period = (me * rows + rows) // span
    designs = [jnp.full((8, LANE), seq_ref[p], jnp.int32) for p in (period, next_period)]

    def gain_of(level):
        return jnp.where(
            level < 2,
            jnp.where(level == 0, gains[0], gains[1]),
            jnp.where(level == 2, gains[2], gains[3]),
        )

    def gain_tile(source, r, tile, target):
        design = designs[0] if r < own_bands else designs[1]
        maps = [source[k, pl.ds(8 * r, 8), at(tile)] for k in range(source.shape[0])]
        level = maps[0]
        for k in range(1, len(maps)):
            level = jnp.where(design == k, maps[k], level)
        coeff[pl.ds(8 * r, 8), at(target)] = gain_of(level)

    def gain_bands(which):
        def body(tile, carry):
            for r in which:
                gain_tile(design_rows, r, tile, tile + PAD)
            return carry

        lax.fori_loop(0, own, body, 0, unroll=2)
        for r in which:
            gain_tile(edge_rows, r, 0, here)

    def load(ref, r, tile):
        return ref[pl.ds(8 * r, 8), at(tile)]

    def advance(j, s, which, main):
        old, new = state[s - 1], state[s]
        base = CHUNK * j + PAD - s
        ahead_tiles = [[load(old[0], r, base + i) for r in which] for i in range(CHUNK + 1)]
        if main and s == 1:
            ahead_tiles = [
                [jnp.where(last_vec, 0.0, v) if r >= own_bands else v for r, v in zip(which, tile)]
                for tile in ahead_tiles
            ]
        hx_low = [load(new[1], r, base - 1) for r in which]
        cut_low = jnp.full((8, LANE), core * 1024 + j, jnp.int32) == 0
        cut_high = jnp.full((8, LANE), (1 - core) * 1024 + chunks - j, jnp.int32) == 0
        for i in range(CHUNK):
            tile = base + i
            e_now, e_right = ahead_tiles[i], ahead_tiles[i + 1]
            hx_new, hz_new = [], []
            bound = None
            if main:
                row = bound_in[pl.ds(s - 1, 1), at(tile)]
                bound = jnp.where(last_vec, 0.0, jnp.broadcast_to(row, (8, LANE)))
            for k, r in enumerate(which):
                e = e_now[k]
                hx = load(old[1], r, tile)
                hz = load(old[2], r, tile)
                if main and s == 1 and r >= own_bands:
                    hx = jnp.where(last_vec, 0.0, hx)
                    hz = jnp.where(last_vec, 0.0, hz)
                upper = pltpu.roll(jnp.where(lane == 0, e_right[k], e), LANE - 1, 1)
                hx = hx + COURANT * (upper - e)
                following = e_now[k + 1] if k + 1 < len(which) else (bound if main else zero)
                beyond = pltpu.roll(jnp.where(sub == 0, following, e), 7, 0)
                hz = hz - COURANT * (beyond - e)
                if i == s - 1:
                    hx = jnp.where(cut_low, 0.0, hx)
                if main and r < REACH // 8:
                    inside = sub + (me * rows + 8 * r) >= offsets[s - 1]
                    hz = jnp.where(inside, hz, 0.0)
                if main and r >= own_bands:
                    inside = sub + (me * rows + 8 * r) < offsets[s - 1] + count * rows
                    hx = jnp.where(inside, hx, 0.0)
                    hz = jnp.where(inside, hz, 0.0)
                hx_new.append(hx)
                hz_new.append(hz)
            for k, r in enumerate(which):
                e, hx, hz = e_now[k], hx_new[k], hz_new[k]
                lower = pltpu.roll(jnp.where(lane == LANE - 1, hx_low[k], hx), 1, 1)
                before = hz_new[k - 1] if k > 0 else zero
                behind = pltpu.roll(jnp.where(sub == 7, before, hz), 1, 0)
                e = e + load(coeff, r, tile) * ((hx - lower) - (hz - behind))
                if i == s:
                    e = jnp.where(cut_high, 0.0, e)
                if main and r >= own_bands:
                    inside = sub + (me * rows + 8 * r) < offsets[s - 1] + count * rows
                    e = jnp.where(inside, e, 0.0)
                new[0][pl.ds(8 * r, 8), at(tile)] = e
                new[1][pl.ds(8 * r, 8), at(tile)] = hx
                new[2][pl.ds(8 * r, 8), at(tile)] = hz
                if not main and r == REACH // 8:
                    bound_out[pl.ds(s, 1), at(tile)] = e[0:1]
                    if s == 1:
                        bound_out[pl.ds(0, 1), at(tile)] = e_now[k][0:1]
            hx_low = hx_new

    strip = [REACH // 8 - 1, REACH // 8]
    for load_copy in loads:
        load_copy.wait()
    for copy in partner_copies:
        copy.wait_recv()
    gain_bands(strip)

    def strip_chunk(j, carry):
        for s in range(1, ITERS):
            advance(j, s, strip, False)
        return carry

    lax.fori_loop(0, chunks + 1, strip_chunk, 0)
    gain_bands([r for r in range(bands) if r not in strip])
    bound_copy = remote(
        bound_out.at[:, mine], bound_in.at[:, mine], bound_send_sem, bound_recv_sem, to_left
    )
    bound_copy.start()
    for j in range(EARLY, chunks):
        for f in range(3):
            chunk_copy(f, j).start()

    relays = [
        remote(
            start[f].at[pl.ds(rows, REACH), at(edge + PAD)],
            start[f].at[pl.ds(rows, REACH), at(halo)],
            relay_send.at[f],
            relay_recv.at[f],
            to_partner,
        )
        for f in range(3)
    ]
    relays.append(
        remote(
            bound_in.at[:, at(edge + PAD)],
            bound_in.at[:, at(halo)],
            relay_send.at[3],
            relay_recv.at[3],
            to_partner,
        )
    )
    for f in range(3):
        edge_copies[f].wait_recv()
        relays[f].start()
    bound_copy.wait_recv()
    relays[3].start()
    for copy in relays:
        copy.wait_recv()

    moved = offsets[-1]
    turn = jnp.bitwise_and(moved, 7)
    back = jnp.bitwise_and(8 - turn, 7)
    moved_vec = jnp.full((8, LANE), moved, jnp.int32)
    turned = sub < jnp.full((8, LANE), turn, jnp.int32)
    everything = list(range(bands))
    outs = (e_out, hx_out, hz_out)

    def finish(j):
        for i in range(CHUNK):
            tile = CHUNK * j + PAD - ITERS + i
            for f in range(3):
                lines = [load(state[ITERS][f], r, tile) for r in range(bands)]
                for k in range(1, REACH // 8 + 1):
                    lines = [
                        jnp.where(moved_vec >= 8 * k, lines[r + 1], lines[r]) if r + 1 < bands else lines[r]
                        for r in range(bands)
                    ]
                for r in range(own_bands):
                    joined = jnp.where(turned, lines[r + 1], lines[r])
                    outs[f][pl.ds(8 * r, 8), at(tile - PAD)] = pltpu.roll(joined, back, 0)

    def main_chunk(j):
        for s in range(1, ITERS + 1):
            advance(j, s, everything, True)

    def first_chunk():
        for f in range(3):
            chunk_copy(f, 0).wait_recv()
        main_chunk(jnp.int32(0))

    def middle(j, carry):
        for f in range(3):
            chunk_copy(f, j).wait_recv()
        main_chunk(j)
        finish(j)
        return carry

    first_chunk()
    lax.fori_loop(1, chunks - 1, middle, 0)
    for f in range(3):
        chunk_copy(f, chunks - 1).wait_recv()

    def closing(j, carry):
        main_chunk(j)
        finish(j)
        return carry

    lax.fori_loop(chunks - 1, chunks + 1, closing, 0)

    for copy in edge_copies + partner_copies + relays + [bound_copy]:
        copy.wait_send()
    for j in range(chunks):
        for f in range(3):
            chunk_copy(f, j).wait_send()


def body(electric, magnetic_x, magnetic_z, index_map, period_seq, eps_table, shifts):
    rows, cells = electric.shape
    own = cells // LANE
    width = (PAD + own + CHUNK) * LANE
    total = rows + REACH
    chunks = own // CHUNK
    types, span, _ = index_map.shape
    field = pltpu.VMEM((total, width), jnp.float32)
    dma = pltpu.SemaphoreType.DMA
    hbm = pl.BlockSpec(memory_space=pl.ANY)
    smem = pl.BlockSpec(memory_space=pltpu.SMEM)
    vmem = pl.BlockSpec(memory_space=pltpu.VMEM)
    out = jax.ShapeDtypeStruct((rows, cells), jnp.float32)
    return pl.pallas_call(
        functools.partial(kernel, rows, own, span),
        out_shape=(out, out, out),
        in_specs=[smem, smem, smem, hbm, hbm, hbm, hbm],
        out_specs=(vmem, vmem, vmem),
        scratch_shapes=[field] * 16
        + [
            pltpu.VMEM((types, total, cells), jnp.int32),
            pltpu.VMEM((types, total, LANE), jnp.int32),
            pltpu.VMEM((ITERS, width), jnp.float32),
            pltpu.VMEM((ITERS, width), jnp.float32),
            dma((5,)),
            dma((5,)),
            dma((5,)),
            dma((3, chunks + 1)),
            dma((3, chunks + 1)),
            dma,
            dma,
            dma((4,)),
            dma((4,)),
        ],
        compiler_params=pltpu.CompilerParams(
            collective_id=0, has_side_effects=True, vmem_limit_bytes=48 * 1024 * 1024
        ),
        name="yee",
    )(shifts, period_seq, eps_table, electric, magnetic_x, magnetic_z, index_map)


def solution(mesh):
    field = P(("grp", "gx"), "gz")
    placed = (field, field, field, P(None, None, "gz"), P("grp"), P(), P("grp"))
    return jax.shard_map(
        body, mesh=mesh, in_specs=placed, out_specs=(field, field, field), check_vma=False
    )
```

```python
import functools
import math

import jax
import jax.numpy as jnp
from jax import lax
from jax.experimental import pallas as pl
from jax.experimental.pallas import tpu as pltpu
from jax.sharding import PartitionSpec as P

ITERS = 4
SMAX = 4
COURANT = 0.6
MESH = pl.DeviceIdType.MESH

LANE = 128
PAD = 5
CHUNK = 4
REACH = ITERS * SMAX
FIRST_HOP, LAST_HOP = 3, 6
EARLY = 6


def kernel(
    rows,
    own,
    span,
    shifts_in,
    seq_in,
    eps_in,
    e_in,
    hx_in,
    hz_in,
    map_in,
    e_out,
    hx_out,
    hz_out,
    e0,
    hx0,
    hz0,
    e1,
    hx1,
    hz1,
    e2,
    hx2,
    hz2,
    e3,
    hx3,
    hz3,
    e4,
    hx4,
    hz4,
    coeff,
    design_rows,
    edge_rows,
    bound_out,
    bound_in,
    shifts_ref,
    seq_ref,
    eps_ref,
    scalar_sem,
    local_sem,
    edge_send,
    edge_recv,
    send_sem,
    recv_sem,
    bound_send_sem,
    bound_recv_sem,
    relay_send,
    relay_recv,
    stage_e,
    stage_hx,
    stage_hz,
    stage_bound,
    stage_recv,
    stage_bound_recv,
    forward_send,
    forward_bound_send,
    ahead_sem,
):
    me = lax.axis_index("gx")
    core = lax.axis_index("gz")
    count = lax.axis_size("gx")
    left = lax.rem(me + count - 1, count)
    right = lax.rem(me + 1, count)
    total = rows + REACH
    bands = total // 8
    own_bands = rows // 8
    chunks = own // CHUNK
    cells = own * LANE
    is_last = me == count - 1

    to_left = {"gx": left}
    to_right = {"gx": right}
    to_partner = {"gz": 1 - core}

    ins = (e_in, hx_in, hz_in)
    state = ((e0, hx0, hz0), (e1, hx1, hz1), (e2, hx2, hz2), (e3, hx3, hz3), (e4, hx4, hz4))
    start = state[0]
    mine = pl.ds(PAD * LANE, cells)

    def at(tile):
        return pl.ds(pl.multiple_of(tile * LANE, LANE), LANE)

    phase = lax.rem(me * rows, span)
    high = lax.rem(me * rows + rows, span)
    loads = [
        pltpu.make_async_copy(ins[f], start[f].at[pl.ds(0, rows), mine], local_sem.at[f])
        for f in range(3)
    ]
    loads.append(
        pltpu.make_async_copy(
            map_in.at[:, pl.ds(pl.multiple_of(phase, 8), rows), :],
            design_rows.at[:, pl.ds(0, rows), :],
            local_sem.at[3],
        )
    )
    loads.append(
        pltpu.make_async_copy(
            map_in.at[:, pl.ds(pl.multiple_of(high, 8), REACH), :],
            design_rows.at[:, pl.ds(rows, REACH), :],
            local_sem.at[4],
        )
    )
    scalars = [
        pltpu.make_async_copy(source, target, scalar_sem.at[k])
        for k, (source, target) in enumerate(
            ((shifts_in, shifts_ref), (seq_in, seq_ref), (eps_in, eps_ref))
        )
    ]
    for copy in scalars + loads:
        copy.start()

    side = math.isqrt(count)
    place = lax.rem(me, side)
    sends = me > 0
    receives = me < count - 1
    staged = sends & ((place == 0) | ((me == 1) & (core == 0)))
    direct = sends & ~staged
    fed = me < count - side
    hop_first = fed & (place == FIRST_HOP)
    hop_last = (fed & (place == LAST_HOP)) | ((me == 0) & (core == 1))
    hops = hop_first | hop_last
    stage_target = {
        "gx": jnp.where(me == 1, 0, me - side + FIRST_HOP),
        "gz": jnp.where(me == 1, 1, core),
    }
    next_target = {"gx": me + (LAST_HOP - FIRST_HOP)}
    last_target = {
        "gx": jnp.where(me == 0, 0, me + (side - 1 - LAST_HOP)),
        "gz": jnp.where(me == 0, 0, core),
    }
    flow_core = jnp.where(me == 0, 0, core)

    barrier = pltpu.get_barrier_semaphore()

    def greet(condition, target):
        @pl.when(condition)
        def _():
            pl.semaphore_signal(barrier, inc=1, device_id=target, device_id_type=MESH)

    greet(receives & (place < side - 1) & (me > 0), to_right)
    greet((me == 0) & (core == 1), {"gx": 1, "gz": 0})
    greet((me == 0) & (core == 1), {"gx": 1, "gz": 1})
    greet(hop_first, {"gx": me + side - FIRST_HOP})
    pl.semaphore_signal(barrier, inc=1, device_id=to_partner, device_id_type=MESH)

    @pl.when(sends)
    def _():
        pl.semaphore_wait(barrier, 2)

    @pl.when(~sends)
    def _():
        pl.semaphore_wait(barrier, 1)

    def tell(condition):
        @pl.when(condition)
        def _():
            pl.semaphore_signal(ahead_sem, inc=1, device_id=to_left, device_id_type=MESH)

    tell(fed & ((place == side - 1) | (place == LAST_HOP)))

    edge = (1 - core) * (own - 1)
    halo = jnp.where(core == 1, PAD + own, PAD - 1)
    here = jnp.where(core == 0, PAD + own, PAD - 1)
    outside = jnp.where(core == 1, PAD + own, PAD - 1)

    def remote(src, dst, send, recv, target):
        return pltpu.make_async_remote_copy(
            src_ref=src, dst_ref=dst, send_sem=send, recv_sem=recv, device_id=target, device_id_type=MESH
        )

    stages = (stage_e, stage_hx, stage_hz)

    def columns(flow, slot, shift):
        if isinstance(slot, int) and slot == chunks:
            first, tiles = (1 - flow) * (own - 1), 1
        else:
            tiles = CHUNK - 1 if isinstance(slot, int) and slot == chunks - 1 else CHUNK
            first = flow + slot * CHUNK
        return pl.ds(pl.multiple_of((first + shift) * LANE, LANE), tiles * LANE)

    def piece(f, slot, kind, handed=False):
        flow = flow_core if handed else core
        here_at = columns(flow, slot, 0)
        source = stages[f].at[:, here_at] if handed else ins[f].at[pl.ds(0, REACH), here_at]
        if kind == "direct":
            target = start[f].at[pl.ds(rows, REACH), columns(flow, slot, PAD)]
            device = last_target if handed else to_left
            arrived = recv_sem
        else:
            target = stages[f].at[:, here_at]
            device = next_target if handed else stage_target
            arrived = stage_recv
        sent = forward_send if handed else send_sem
        return remote(source, target, sent.at[f, slot], arrived.at[f, slot], device)

    def bound_piece(kind, handed=False):
        source = stage_bound if handed else bound_out.at[:, mine]
        sent = forward_bound_send if handed else bound_send_sem
        if kind == "direct":
            device = last_target if handed else to_left
            return remote(source, bound_in.at[:, mine], sent, bound_recv_sem, device)
        device = next_target if handed else stage_target
        return remote(source, stage_bound, sent, stage_bound_recv, device)

    def send(slots, bound=False):
        for condition, kind in ((direct, "direct"), (staged, "stage")):

            @pl.when(condition)
            def _(kind=kind):
                if bound:
                    bound_piece(kind).start()
                for slot in slots:
                    for f in range(3):
                        piece(f, slot, kind).start()

    def hand_on(slots, bound=False):
        for condition, kind in ((hop_first, "stage"), (hop_last, "direct")):

            @pl.when(condition)
            def _(kind=kind):
                for slot in slots:
                    for f in range(3):
                        piece(f, slot, "stage", True).wait_recv()
                        piece(f, slot, kind, True).start()
                if bound:
                    bound_piece("stage", True).wait_recv()
                    bound_piece(kind, True).start()

    partner_copies = [
        remote(
            ins[f].at[:, at(edge)],
            start[f].at[pl.ds(0, rows), at(halo)],
            edge_send.at[f],
            edge_recv.at[f],
            to_partner,
        )
        for f in range(3)
    ]
    partner_copies.append(
        remote(
            map_in.at[:, pl.ds(pl.multiple_of(phase, 8), rows), at(edge)],
            edge_rows.at[:, pl.ds(0, rows), :],
            edge_send.at[3],
            edge_recv.at[3],
            to_partner,
        )
    )
    partner_copies.append(
        remote(
            map_in.at[:, pl.ds(pl.multiple_of(high, 8), REACH), at(edge)],
            edge_rows.at[:, pl.ds(rows, REACH), :],
            edge_send.at[4],
            edge_recv.at[4],
            to_partner,
        )
    )
    for copy in partner_copies:
        copy.start()
    send([chunks] + list(range(EARLY)))

    between = fed & (place > FIRST_HOP) & (place < LAST_HOP)

    @pl.when(between)
    def _():
        pl.semaphore_wait(ahead_sem, 1)

    tell(between)
    for copy in scalars:
        copy.wait()

    lane = lax.broadcasted_iota(jnp.int32, (8, LANE), 1)
    sub = lax.broadcasted_iota(jnp.int32, (8, LANE), 0)
    zero = jnp.zeros((8, LANE), jnp.float32)
    last_vec = jnp.full((8, LANE), me, jnp.int32) == count - 1
    offsets = []
    offset = jnp.int32(0)
    for step in range(ITERS):
        offset = offset + shifts_ref[step]
        offsets.append(offset)

    for f in range(3):
        for r in range(bands):
            start[f][pl.ds(8 * r, 8), at(outside)] = zero

    gains = [COURANT * (1.0 / jnp.full((8, LANE), eps_ref[k], jnp.float32)) for k in range(4)]
    period = me * rows // span
    next_period = (me * rows + rows) // span
    designs = [jnp.full((8, LANE), seq_ref[p], jnp.int32) for p in (period, next_period)]

    def gain_of(level):
        return jnp.where(
            level < 2,
            jnp.where(level == 0, gains[0], gains[1]),
            jnp.where(level == 2, gains[2], gains[3]),
        )

    def gain_tile(source, r, tile, target):
        design = designs[0] if r < own_bands else designs[1]
        maps = [source[k, pl.ds(8 * r, 8), at(tile)] for k in range(source.shape[0])]
        level = maps[0]
        for k in range(1, len(maps)):
            level = jnp.where(design == k, maps[k], level)
        coeff[pl.ds(8 * r, 8), at(target)] = gain_of(level)

    def gain_bands(which):
        def body(tile, carry):
            for r in which:
                gain_tile(design_rows, r, tile, tile + PAD)
            return carry

        lax.fori_loop(0, own, body, 0, unroll=2)
        for r in which:
            gain_tile(edge_rows, r, 0, here)

    def load(ref, r, tile):
        return ref[pl.ds(8 * r, 8), at(tile)]

    def advance(j, s, which, main):
        old, new = state[s - 1], state[s]
        base = CHUNK * j + PAD - s
        ahead_tiles = [[load(old[0], r, base + i) for r in which] for i in range(CHUNK + 1)]
        if main and s == 1:
            ahead_tiles = [
                [jnp.where(last_vec, 0.0, v) if r >= own_bands else v for r, v in zip(which, tile)]
                for tile in ahead_tiles
            ]
        hx_low = [load(new[1], r, base - 1) for r in which]
        cut_low = jnp.full((8, LANE), core * 1024 + j, jnp.int32) == 0
        cut_high = jnp.full((8, LANE), (1 - core) * 1024 + chunks - j, jnp.int32) == 0
        for i in range(CHUNK):
            tile = base + i
            e_now, e_right = ahead_tiles[i], ahead_tiles[i + 1]
            hx_new, hz_new = [], []
            bound = None
            if main:
                row = bound_in[pl.ds(s - 1, 1), at(tile)]
                bound = jnp.where(last_vec, 0.0, jnp.broadcast_to(row, (8, LANE)))
            for k, r in enumerate(which):
                e = e_now[k]
                hx = load(old[1], r, tile)
                hz = load(old[2], r, tile)
                if main and s == 1 and r >= own_bands:
                    hx = jnp.where(last_vec, 0.0, hx)
                    hz = jnp.where(last_vec, 0.0, hz)
                upper = pltpu.roll(jnp.where(lane == 0, e_right[k], e), LANE - 1, 1)
                hx = hx + COURANT * (upper - e)
                following = e_now[k + 1] if k + 1 < len(which) else (bound if main else zero)
                beyond = pltpu.roll(jnp.where(sub == 0, following, e), 7, 0)
                hz = hz - COURANT * (beyond - e)
                if i == s - 1:
                    hx = jnp.where(cut_low, 0.0, hx)
                if main and r < REACH // 8:
                    inside = sub + (me * rows + 8 * r) >= offsets[s - 1]
                    hz = jnp.where(inside, hz, 0.0)
                if main and r >= own_bands:
                    inside = sub + (me * rows + 8 * r) < offsets[s - 1] + count * rows
                    hx = jnp.where(inside, hx, 0.0)
                    hz = jnp.where(inside, hz, 0.0)
                hx_new.append(hx)
                hz_new.append(hz)
            for k, r in enumerate(which):
                e, hx, hz = e_now[k], hx_new[k], hz_new[k]
                lower = pltpu.roll(jnp.where(lane == LANE - 1, hx_low[k], hx), 1, 1)
                before = hz_new[k - 1] if k > 0 else zero
                behind = pltpu.roll(jnp.where(sub == 7, before, hz), 1, 0)
                e = e + load(coeff, r, tile) * ((hx - lower) - (hz - behind))
                if i == s:
                    e = jnp.where(cut_high, 0.0, e)
                if main and r >= own_bands:
                    inside = sub + (me * rows + 8 * r) < offsets[s - 1] + count * rows
                    e = jnp.where(inside, e, 0.0)
                new[0][pl.ds(8 * r, 8), at(tile)] = e
                new[1][pl.ds(8 * r, 8), at(tile)] = hx
                new[2][pl.ds(8 * r, 8), at(tile)] = hz
                if not main and r == REACH // 8:
                    bound_out[pl.ds(s, 1), at(tile)] = e[0:1]
                    if s == 1:
                        bound_out[pl.ds(0, 1), at(tile)] = e_now[k][0:1]
            hx_low = hx_new

    strip = [REACH // 8 - 1, REACH // 8]
    for load_copy in loads:
        load_copy.wait()
    for copy in partner_copies:
        copy.wait_recv()
    gain_bands(strip)

    def strip_chunk(j, carry):
        for s in range(1, ITERS):
            advance(j, s, strip, False)
        return carry

    @pl.when(sends)
    def _():
        lax.fori_loop(0, chunks + 1, strip_chunk, 0)

    gain_bands([r for r in range(bands) if r not in strip])
    send(range(EARLY, chunks), bound=True)

    @pl.when(fed & ((place == FIRST_HOP) | (place == LAST_HOP)))
    def _():
        pl.semaphore_wait(ahead_sem, 1)

    hand_on([chunks] + list(range(EARLY)), bound=True)

    relays = [
        remote(
            start[f].at[pl.ds(rows, REACH), at(edge + PAD)],
            start[f].at[pl.ds(rows, REACH), at(halo)],
            relay_send.at[f],
            relay_recv.at[f],
            to_partner,
        )
        for f in range(3)
    ]
    relays.append(
        remote(
            bound_in.at[:, at(edge + PAD)],
            bound_in.at[:, at(halo)],
            relay_send.at[3],
            relay_recv.at[3],
            to_partner,
        )
    )

    @pl.when(receives)
    def _():
        for f in range(3):
            piece(f, chunks, "direct").wait_recv()
            relays[f].start()
        bound_piece("direct").wait_recv()
        relays[3].start()
        for copy in relays:
            copy.wait_recv()

    moved = offsets[-1]
    turn = jnp.bitwise_and(moved, 7)
    back = jnp.bitwise_and(8 - turn, 7)
    moved_vec = jnp.full((8, LANE), moved, jnp.int32)
    turned = sub < jnp.full((8, LANE), turn, jnp.int32)
    everything = list(range(bands))
    outs = (e_out, hx_out, hz_out)

    def finish(j):
        for i in range(CHUNK):
            tile = CHUNK * j + PAD - ITERS + i
            for f in range(3):
                lines = [load(state[ITERS][f], r, tile) for r in range(bands)]
                for k in range(1, REACH // 8 + 1):
                    lines = [
                        jnp.where(moved_vec >= 8 * k, lines[r + 1], lines[r]) if r + 1 < bands else lines[r]
                        for r in range(bands)
                    ]
                for r in range(own_bands):
                    joined = jnp.where(turned, lines[r + 1], lines[r])
                    outs[f][pl.ds(8 * r, 8), at(tile - PAD)] = pltpu.roll(joined, back, 0)

    def main_chunk(j):
        for s in range(1, ITERS + 1):
            advance(j, s, everything, True)

    def arrive(j):
        @pl.when(receives)
        def _():
            for f in range(3):
                piece(f, j, "direct").wait_recv()

    def middle(j, carry):
        arrive(j)
        main_chunk(j)
        finish(j)
        return carry

    arrive(0)
    main_chunk(jnp.int32(0))
    lax.fori_loop(1, EARLY, middle, 0)
    for j in range(EARLY, chunks - 1):
        hand_on([j])
        middle(jnp.int32(j), 0)
    hand_on([chunks - 1])
    arrive(chunks - 1)

    def closing(j, carry):
        main_chunk(j)
        finish(j)
        return carry

    lax.fori_loop(chunks - 1, chunks + 1, closing, 0)

    for copy in partner_copies:
        copy.wait_send()

    @pl.when(receives)
    def _():
        for copy in relays:
            copy.wait_send()

    for condition, handed in ((sends, False), (hops, True)):

        @pl.when(condition)
        def _(handed=handed):
            bound_piece("direct", handed).wait_send()
            for slot in range(chunks + 1):
                for f in range(3):
                    piece(f, slot, "direct", handed).wait_send()


def store(e_in, hx_in, hz_in, e_out, hx_out, hz_out, sem):
    copies = [
        pltpu.make_async_copy(source, target, sem.at[k])
        for k, (source, target) in enumerate(
            ((e_in, e_out), (hx_in, hx_out), (hz_in, hz_out))
        )
    ]
    for copy in copies:
        copy.start()
    for copy in copies:
        copy.wait()


def body(electric, magnetic_x, magnetic_z, index_map, period_seq, eps_table, shifts):
    rows, cells = electric.shape
    own = cells // LANE
    width = (PAD + own + CHUNK) * LANE
    total = rows + REACH
    chunks = own // CHUNK
    types, span, _ = index_map.shape
    field = pltpu.VMEM((total, width), jnp.float32)
    dma = pltpu.SemaphoreType.DMA
    hbm = pl.BlockSpec(memory_space=pltpu.HBM)
    vmem = pl.BlockSpec(memory_space=pltpu.VMEM)
    out = jax.ShapeDtypeStruct((rows, cells), jnp.float32)
    fields = pl.pallas_call(
        functools.partial(kernel, rows, own, span),
        out_shape=(out, out, out),
        in_specs=[hbm] * 7,
        out_specs=(vmem, vmem, vmem),
        scratch_shapes=[field] * 16
        + [
            pltpu.VMEM((types, total, cells), jnp.int32),
            pltpu.VMEM((types, total, LANE), jnp.int32),
            pltpu.VMEM((ITERS, width), jnp.float32),
            pltpu.VMEM((ITERS, width), jnp.float32),
            pltpu.SMEM(shifts.shape, jnp.int32),
            pltpu.SMEM(period_seq.shape, jnp.int32),
            pltpu.SMEM(eps_table.shape, jnp.float32),
            dma((3,)),
            dma((5,)),
            dma((5,)),
            dma((5,)),
            dma((3, chunks + 1)),
            dma((3, chunks + 1)),
            dma,
            dma,
            dma((4,)),
            dma((4,)),
        ]
        + [pltpu.VMEM((REACH, cells), jnp.float32)] * 3
        + [
            pltpu.VMEM((ITERS, cells), jnp.float32),
            dma((3, chunks + 1)),
            dma,
            dma((3, chunks + 1)),
            dma,
            pltpu.SemaphoreType.REGULAR,
        ],
        compiler_params=pltpu.CompilerParams(
            collective_id=0, has_side_effects=True, vmem_limit_bytes=48 * 1024 * 1024
        ),
        name="yee",
    )(
        *(
            pltpu.with_memory_space_constraint(x, pltpu.HBM)
            for x in (shifts, period_seq, eps_table, electric, magnetic_x, magnetic_z, index_map)
        )
    )
    return pl.pallas_call(
        store,
        out_shape=(out, out, out),
        in_specs=[pl.BlockSpec(memory_space=pl.ANY)] * 3,
        out_specs=[hbm] * 3,
        scratch_shapes=[dma((3,))],
        compiler_params=pltpu.CompilerParams(vmem_limit_bytes=1024 * 1024),
        name="store",
    )(*fields)


def solution(mesh):
    field = P(("grp", "gx"), "gz")
    placed = (field, field, field, P(None, None, "gz"), P("grp"), P(), P("grp"))
    return jax.shard_map(
        body, mesh=mesh, in_specs=placed, out_specs=(field, field, field), check_vma=False
    )
```

```python
import functools
import math

import jax
import jax.numpy as jnp
from jax import lax
from jax.experimental import pallas as pl
from jax.experimental.pallas import tpu as pltpu
from jax.sharding import PartitionSpec as P

ITERS = 4
SMAX = 4
COURANT = 0.6
MESH = pl.DeviceIdType.MESH

LANE = 128
PAD = 5
CHUNK = 4
REACH = ITERS * SMAX
FIRST_HOP, LAST_HOP = 3, 6
HANDED = 4
EARLY = 6


def kernel(
    rows,
    own,
    span,
    shifts_in,
    seq_in,
    eps_in,
    e_in,
    hx_in,
    hz_in,
    map_in,
    e_out,
    hx_out,
    hz_out,
    e0,
    hx0,
    hz0,
    e1,
    hx1,
    hz1,
    e2,
    hx2,
    hz2,
    e3,
    hx3,
    hz3,
    e4,
    hx4,
    hz4,
    coeff,
    design_rows,
    edge_rows,
    bound_out,
    bound_in,
    shifts_ref,
    seq_ref,
    eps_ref,
    scalar_sem,
    local_sem,
    edge_send,
    edge_recv,
    send_sem,
    recv_sem,
    bound_send_sem,
    bound_recv_sem,
    relay_send,
    relay_recv,
    stage_e,
    stage_hx,
    stage_hz,
    stage_bound,
    stage_recv,
    stage_bound_recv,
    forward_send,
    forward_bound_send,
    ahead_sem,
):
    me = lax.axis_index("gx")
    core = lax.axis_index("gz")
    count = lax.axis_size("gx")
    left = lax.rem(me + count - 1, count)
    right = lax.rem(me + 1, count)
    total = rows + REACH
    bands = total // 8
    own_bands = rows // 8
    chunks = own // CHUNK
    cells = own * LANE
    is_last = me == count - 1

    to_left = {"gx": left}
    to_right = {"gx": right}
    to_partner = {"gz": 1 - core}

    ins = (e_in, hx_in, hz_in)
    state = ((e0, hx0, hz0), (e1, hx1, hz1), (e2, hx2, hz2), (e3, hx3, hz3), (e4, hx4, hz4))
    start = state[0]
    mine = pl.ds(PAD * LANE, cells)

    def at(tile):
        return pl.ds(pl.multiple_of(tile * LANE, LANE), LANE)

    phase = lax.rem(me * rows, span)
    high = lax.rem(me * rows + rows, span)
    loads = [
        pltpu.make_async_copy(ins[f], start[f].at[pl.ds(0, rows), mine], local_sem.at[f])
        for f in range(3)
    ]
    loads.append(
        pltpu.make_async_copy(
            map_in.at[:, pl.ds(pl.multiple_of(phase, 8), rows), :],
            design_rows.at[:, pl.ds(0, rows), :],
            local_sem.at[3],
        )
    )
    loads.append(
        pltpu.make_async_copy(
            map_in.at[:, pl.ds(pl.multiple_of(high, 8), REACH), :],
            design_rows.at[:, pl.ds(rows, REACH), :],
            local_sem.at[4],
        )
    )
    scalars = [
        pltpu.make_async_copy(source, target, scalar_sem.at[k])
        for k, (source, target) in enumerate(
            ((shifts_in, shifts_ref), (seq_in, seq_ref), (eps_in, eps_ref))
        )
    ]
    for copy in scalars + loads:
        copy.start()

    side = math.isqrt(count)
    place = lax.rem(me, side)
    sends = me > 0
    receives = me < count - 1
    through = (me == 1) & (core == 0)
    direct = sends & ~through
    crossing = sends & (place == 0)
    hop_start = (me == 0) & (core == 1)
    hop_first = (me >= side) & (place == FIRST_HOP)
    hop_last = (me >= side) & (place == LAST_HOP)
    stage_target = {
        "gx": jnp.where(me == 1, 0, me + FIRST_HOP),
        "gz": jnp.where(me == 1, 1, core),
    }
    next_target = {"gx": me + (LAST_HOP - FIRST_HOP)}
    last_target = {
        "gx": jnp.where(me == 0, 0, me - LAST_HOP - 1),
        "gz": jnp.where(me == 0, 0, core),
    }
    flow_core = jnp.where(me == 0, 0, core)

    barrier = pltpu.get_barrier_semaphore()

    def greet(condition, target):
        @pl.when(condition)
        def _():
            pl.semaphore_signal(barrier, inc=1, device_id=target, device_id_type=MESH)

    greet(receives & (me > 0), to_right)
    greet(hop_start, {"gx": 1, "gz": 0})
    greet(hop_start, {"gx": 1, "gz": 1})
    greet(hop_first, {"gx": me - FIRST_HOP})
    row_end = (me >= side) & (place == side - 1)
    greet(receives & (place == side - 1), {"gx": me + side})
    pl.semaphore_signal(barrier, inc=1, device_id=to_partner, device_id_type=MESH)

    for condition, amount in (
        (~sends, 1),
        (sends & ~(crossing | row_end), 2),
        (crossing | row_end, 3),
    ):

        @pl.when(condition)
        def _(amount=amount):
            pl.semaphore_wait(barrier, amount)

    def tell(condition):
        @pl.when(condition)
        def _():
            pl.semaphore_signal(ahead_sem, inc=1, device_id=to_left, device_id_type=MESH)

    tell(hop_last | row_end)

    edge = (1 - core) * (own - 1)
    halo = jnp.where(core == 1, PAD + own, PAD - 1)
    here = jnp.where(core == 0, PAD + own, PAD - 1)
    outside = jnp.where(core == 1, PAD + own, PAD - 1)

    def remote(src, dst, send, recv, target):
        return pltpu.make_async_remote_copy(
            src_ref=src, dst_ref=dst, send_sem=send, recv_sem=recv, device_id=target, device_id_type=MESH
        )

    stages = (stage_e, stage_hx, stage_hz)

    def columns(flow, slot, shift):
        if isinstance(slot, int) and slot == chunks:
            first, tiles = (1 - flow) * (own - 1), 1
        else:
            tiles = CHUNK - 1 if isinstance(slot, int) and slot == chunks - 1 else CHUNK
            first = flow + slot * CHUNK
        return pl.ds(pl.multiple_of((first + shift) * LANE, LANE), tiles * LANE)

    def piece(f, slot, kind, handed=False):
        flow = flow_core if handed else core
        here_at = columns(flow, slot, 0)
        source = stages[f].at[:, here_at] if handed else ins[f].at[pl.ds(0, REACH), here_at]
        if kind == "direct":
            target = start[f].at[pl.ds(rows, REACH), columns(flow, slot, PAD)]
            device = last_target if handed else to_left
            arrived = recv_sem
        else:
            target = stages[f].at[:, here_at]
            device = next_target if handed else stage_target
            arrived = stage_recv
        sent = forward_send if handed else send_sem
        return remote(source, target, sent.at[f, slot], arrived.at[f, slot], device)

    def bound_piece(kind, handed=False):
        source = stage_bound if handed else bound_out.at[:, mine]
        sent = forward_bound_send if handed else bound_send_sem
        if kind == "direct":
            device = last_target if handed else to_left
            return remote(source, bound_in.at[:, mine], sent, bound_recv_sem, device)
        device = next_target if handed else stage_target
        return remote(source, stage_bound, sent, stage_bound_recv, device)

    def send(slots, bound=False):
        if bound:
            for condition, kind in ((direct, "direct"), (through, "stage")):

                @pl.when(condition)
                def _(kind=kind):
                    bound_piece(kind).start()

        for slot in slots:
            whole = slot == chunks or slot < HANDED
            for condition, kind in (
                (direct if whole else direct & ~crossing, "direct"),
                (through if whole else through | crossing, "stage"),
            ):

                @pl.when(condition)
                def _(kind=kind, slot=slot):
                    for f in range(3):
                        piece(f, slot, kind).start()

    def hand_on(condition, kind, slots, bound=False):
        @pl.when(condition)
        def _():
            for slot in slots:
                for f in range(3):
                    piece(f, slot, "stage", True).wait_recv()
                    piece(f, slot, kind, True).start()
            if bound:
                bound_piece("stage", True).wait_recv()
                bound_piece(kind, True).start()

    partner_copies = [
        remote(
            ins[f].at[:, at(edge)],
            start[f].at[pl.ds(0, rows), at(halo)],
            edge_send.at[f],
            edge_recv.at[f],
            to_partner,
        )
        for f in range(3)
    ]
    partner_copies.append(
        remote(
            map_in.at[:, pl.ds(pl.multiple_of(phase, 8), rows), at(edge)],
            edge_rows.at[:, pl.ds(0, rows), :],
            edge_send.at[3],
            edge_recv.at[3],
            to_partner,
        )
    )
    partner_copies.append(
        remote(
            map_in.at[:, pl.ds(pl.multiple_of(high, 8), REACH), at(edge)],
            edge_rows.at[:, pl.ds(rows, REACH), :],
            edge_send.at[4],
            edge_recv.at[4],
            to_partner,
        )
    )
    for copy in partner_copies:
        copy.start()
    send([chunks] + list(range(EARLY)))

    relays = [
        remote(
            start[f].at[pl.ds(rows, REACH), at(edge + PAD)],
            start[f].at[pl.ds(rows, REACH), at(halo)],
            relay_send.at[f],
            relay_recv.at[f],
            to_partner,
        )
        for f in range(3)
    ]
    relays.append(
        remote(
            bound_in.at[:, at(edge + PAD)],
            bound_in.at[:, at(halo)],
            relay_send.at[3],
            relay_recv.at[3],
            to_partner,
        )
    )

    def pass_edge(condition):
        @pl.when(condition)
        def _():
            for f in range(3):
                piece(f, chunks, "direct").wait_recv()
                relays[f].start()
            bound_piece("direct").wait_recv()
            relays[3].start()

    pass_edge(hop_start)
    hand_on(hop_start, "direct", [chunks] + list(range(EARLY)), bound=True)
    between = (me >= side) & (place > FIRST_HOP) & (place < LAST_HOP)

    @pl.when(between)
    def _():
        pl.semaphore_wait(ahead_sem, 1)

    tell(between)
    for copy in scalars:
        copy.wait()

    lane = lax.broadcasted_iota(jnp.int32, (8, LANE), 1)
    sub = lax.broadcasted_iota(jnp.int32, (8, LANE), 0)
    zero = jnp.zeros((8, LANE), jnp.float32)
    last_vec = jnp.full((8, LANE), me, jnp.int32) == count - 1
    offsets = []
    offset = jnp.int32(0)
    for step in range(ITERS):
        offset = offset + shifts_ref[step]
        offsets.append(offset)

    for f in range(3):
        for r in range(bands):
            start[f][pl.ds(8 * r, 8), at(outside)] = zero

    gains = [COURANT * (1.0 / jnp.full((8, LANE), eps_ref[k], jnp.float32)) for k in range(4)]
    period = me * rows // span
    next_period = (me * rows + rows) // span
    designs = [jnp.full((8, LANE), seq_ref[p], jnp.int32) for p in (period, next_period)]

    def gain_of(level):
        return jnp.where(
            level < 2,
            jnp.where(level == 0, gains[0], gains[1]),
            jnp.where(level == 2, gains[2], gains[3]),
        )

    def gain_tile(source, r, tile, target):
        design = designs[0] if r < own_bands else designs[1]
        maps = [source[k, pl.ds(8 * r, 8), at(tile)] for k in range(source.shape[0])]
        level = maps[0]
        for k in range(1, len(maps)):
            level = jnp.where(design == k, maps[k], level)
        coeff[pl.ds(8 * r, 8), at(target)] = gain_of(level)

    def gain_bands(which):
        def body(tile, carry):
            for r in which:
                gain_tile(design_rows, r, tile, tile + PAD)
            return carry

        lax.fori_loop(0, own, body, 0, unroll=2)
        for r in which:
            gain_tile(edge_rows, r, 0, here)

    def load(ref, r, tile):
        return ref[pl.ds(8 * r, 8), at(tile)]

    def advance(j, s, which, main):
        old, new = state[s - 1], state[s]
        base = CHUNK * j + PAD - s
        ahead_tiles = [[load(old[0], r, base + i) for r in which] for i in range(CHUNK + 1)]
        if main and s == 1:
            ahead_tiles = [
                [jnp.where(last_vec, 0.0, v) if r >= own_bands else v for r, v in zip(which, tile)]
                for tile in ahead_tiles
            ]
        hx_low = [load(new[1], r, base - 1) for r in which]
        cut_low = jnp.full((8, LANE), core * 1024 + j, jnp.int32) == 0
        cut_high = jnp.full((8, LANE), (1 - core) * 1024 + chunks - j, jnp.int32) == 0
        for i in range(CHUNK):
            tile = base + i
            e_now, e_right = ahead_tiles[i], ahead_tiles[i + 1]
            hx_new, hz_new = [], []
            bound = None
            if main:
                row = bound_in[pl.ds(s - 1, 1), at(tile)]
                bound = jnp.where(last_vec, 0.0, jnp.broadcast_to(row, (8, LANE)))
            for k, r in enumerate(which):
                e = e_now[k]
                hx = load(old[1], r, tile)
                hz = load(old[2], r, tile)
                if main and s == 1 and r >= own_bands:
                    hx = jnp.where(last_vec, 0.0, hx)
                    hz = jnp.where(last_vec, 0.0, hz)
                upper = pltpu.roll(jnp.where(lane == 0, e_right[k], e), LANE - 1, 1)
                hx = hx + COURANT * (upper - e)
                following = e_now[k + 1] if k + 1 < len(which) else (bound if main else zero)
                beyond = pltpu.roll(jnp.where(sub == 0, following, e), 7, 0)
                hz = hz - COURANT * (beyond - e)
                if i == s - 1:
                    hx = jnp.where(cut_low, 0.0, hx)
                if main and r < REACH // 8:
                    inside = sub + (me * rows + 8 * r) >= offsets[s - 1]
                    hz = jnp.where(inside, hz, 0.0)
                if main and r >= own_bands:
                    inside = sub + (me * rows + 8 * r) < offsets[s - 1] + count * rows
                    hx = jnp.where(inside, hx, 0.0)
                    hz = jnp.where(inside, hz, 0.0)
                hx_new.append(hx)
                hz_new.append(hz)
            for k, r in enumerate(which):
                e, hx, hz = e_now[k], hx_new[k], hz_new[k]
                lower = pltpu.roll(jnp.where(lane == LANE - 1, hx_low[k], hx), 1, 1)
                before = hz_new[k - 1] if k > 0 else zero
                behind = pltpu.roll(jnp.where(sub == 7, before, hz), 1, 0)
                e = e + load(coeff, r, tile) * ((hx - lower) - (hz - behind))
                if i == s:
                    e = jnp.where(cut_high, 0.0, e)
                if main and r >= own_bands:
                    inside = sub + (me * rows + 8 * r) < offsets[s - 1] + count * rows
                    e = jnp.where(inside, e, 0.0)
                new[0][pl.ds(8 * r, 8), at(tile)] = e
                new[1][pl.ds(8 * r, 8), at(tile)] = hx
                new[2][pl.ds(8 * r, 8), at(tile)] = hz
                if not main and r == REACH // 8:
                    bound_out[pl.ds(s, 1), at(tile)] = e[0:1]
                    if s == 1:
                        bound_out[pl.ds(0, 1), at(tile)] = e_now[k][0:1]
            hx_low = hx_new

    strip = [REACH // 8 - 1, REACH // 8]
    for load_copy in loads:
        load_copy.wait()
    for copy in partner_copies:
        copy.wait_recv()
    gain_bands(strip)

    def strip_chunk(j, carry):
        for s in range(1, ITERS):
            advance(j, s, strip, False)
        return carry

    @pl.when(sends)
    def _():
        lax.fori_loop(0, chunks + 1, strip_chunk, 0)

    gain_bands([r for r in range(bands) if r not in strip])
    send(range(EARLY, chunks), bound=True)

    @pl.when(hop_first | hop_last)
    def _():
        pl.semaphore_wait(ahead_sem, 1)

    hand_on(hop_first, "stage", range(HANDED, chunks))
    hand_on(hop_last, "direct", range(HANDED, chunks))

    at_start = (me == 0) & (core == 0)

    pass_edge(receives & (me > 0))

    @pl.when(at_start)
    def _():
        for f in range(3):
            piece(f, chunks, "direct").wait_recv()
        bound_piece("direct").wait_recv()

    @pl.when(receives)
    def _():
        @pl.when(~hop_start)
        def _():
            for copy in relays:
                copy.wait_recv()

        @pl.when(hop_start)
        def _():
            theirs = columns(0, chunks, 0)
            copies = [
                pltpu.make_async_copy(
                    stages[f].at[:, theirs], start[f].at[pl.ds(rows, REACH), at(here)], local_sem.at[f]
                )
                for f in range(3)
            ]
            copies.append(
                pltpu.make_async_copy(
                    stage_bound.at[:, theirs], bound_in.at[:, at(here)], local_sem.at[3]
                )
            )
            for copy in copies:
                copy.start()
            for copy in copies:
                copy.wait()

    moved = offsets[-1]
    turn = jnp.bitwise_and(moved, 7)
    back = jnp.bitwise_and(8 - turn, 7)
    moved_vec = jnp.full((8, LANE), moved, jnp.int32)
    turned = sub < jnp.full((8, LANE), turn, jnp.int32)
    everything = list(range(bands))
    outs = (e_out, hx_out, hz_out)

    def finish(j):
        for i in range(CHUNK):
            tile = CHUNK * j + PAD - ITERS + i
            for f in range(3):
                lines = [load(state[ITERS][f], r, tile) for r in range(bands)]
                for k in range(1, REACH // 8 + 1):
                    lines = [
                        jnp.where(moved_vec >= 8 * k, lines[r + 1], lines[r]) if r + 1 < bands else lines[r]
                        for r in range(bands)
                    ]
                for r in range(own_bands):
                    joined = jnp.where(turned, lines[r + 1], lines[r])
                    outs[f][pl.ds(8 * r, 8), at(tile - PAD)] = pltpu.roll(joined, back, 0)

    def main_chunk(j):
        for s in range(1, ITERS + 1):
            advance(j, s, everything, True)

    def arrive(j):
        @pl.when(receives)
        def _():
            for f in range(3):
                piece(f, j, "direct").wait_recv()

    def middle(j, carry):
        arrive(j)
        main_chunk(j)
        finish(j)
        return carry

    arrive(0)
    main_chunk(jnp.int32(0))
    lax.fori_loop(1, EARLY, middle, 0)
    for j in range(EARLY, chunks - 1):
        hand_on(hop_start, "direct", [j])
        middle(jnp.int32(j), 0)
    hand_on(hop_start, "direct", [chunks - 1])
    arrive(chunks - 1)

    def closing(j, carry):
        main_chunk(j)
        finish(j)
        return carry

    lax.fori_loop(chunks - 1, chunks + 1, closing, 0)

    for copy in partner_copies:
        copy.wait_send()

    @pl.when(receives & ~at_start)
    def _():
        for copy in relays:
            copy.wait_send()

    def drain(condition, handed, slots, bound):
        @pl.when(condition)
        def _():
            if bound:
                bound_piece("direct", handed).wait_send()
            for slot in slots:
                for f in range(3):
                    piece(f, slot, "direct", handed).wait_send()

    drain(sends, False, range(chunks + 1), True)
    drain(hop_start, True, range(chunks + 1), True)
    drain(hop_first | hop_last, True, range(HANDED, chunks), False)


def store(e_in, hx_in, hz_in, e_out, hx_out, hz_out, sem):
    copies = [
        pltpu.make_async_copy(source, target, sem.at[k])
        for k, (source, target) in enumerate(
            ((e_in, e_out), (hx_in, hx_out), (hz_in, hz_out))
        )
    ]
    for copy in copies:
        copy.start()
    for copy in copies:
        copy.wait()


def body(electric, magnetic_x, magnetic_z, index_map, period_seq, eps_table, shifts):
    rows, cells = electric.shape
    own = cells // LANE
    width = (PAD + own + CHUNK) * LANE
    total = rows + REACH
    chunks = own // CHUNK
    types, span, _ = index_map.shape
    field = pltpu.VMEM((total, width), jnp.float32)
    dma = pltpu.SemaphoreType.DMA
    hbm = pl.BlockSpec(memory_space=pltpu.HBM)
    vmem = pl.BlockSpec(memory_space=pltpu.VMEM)
    out = jax.ShapeDtypeStruct((rows, cells), jnp.float32)
    fields = pl.pallas_call(
        functools.partial(kernel, rows, own, span),
        out_shape=(out, out, out),
        in_specs=[hbm] * 7,
        out_specs=(vmem, vmem, vmem),
        scratch_shapes=[field] * 16
        + [
            pltpu.VMEM((types, total, cells), jnp.int32),
            pltpu.VMEM((types, total, LANE), jnp.int32),
            pltpu.VMEM((ITERS, width), jnp.float32),
            pltpu.VMEM((ITERS, width), jnp.float32),
            pltpu.SMEM(shifts.shape, jnp.int32),
            pltpu.SMEM(period_seq.shape, jnp.int32),
            pltpu.SMEM(eps_table.shape, jnp.float32),
            dma((3,)),
            dma((5,)),
            dma((5,)),
            dma((5,)),
            dma((3, chunks + 1)),
            dma((3, chunks + 1)),
            dma,
            dma,
            dma((4,)),
            dma((4,)),
        ]
        + [pltpu.VMEM((REACH, cells), jnp.float32)] * 3
        + [
            pltpu.VMEM((ITERS, cells), jnp.float32),
            dma((3, chunks + 1)),
            dma,
            dma((3, chunks + 1)),
            dma,
            pltpu.SemaphoreType.REGULAR,
        ],
        compiler_params=pltpu.CompilerParams(
            collective_id=0, has_side_effects=True, vmem_limit_bytes=48 * 1024 * 1024
        ),
        name="yee",
    )(
        *(
            pltpu.with_memory_space_constraint(x, pltpu.HBM)
            for x in (shifts, period_seq, eps_table, electric, magnetic_x, magnetic_z, index_map)
        )
    )
    return pl.pallas_call(
        store,
        out_shape=(out, out, out),
        in_specs=[pl.BlockSpec(memory_space=pl.ANY)] * 3,
        out_specs=[hbm] * 3,
        scratch_shapes=[dma((3,))],
        compiler_params=pltpu.CompilerParams(vmem_limit_bytes=1024 * 1024),
        name="store",
    )(*fields)


def solution(mesh):
    field = P(("grp", "gx"), "gz")
    placed = (field, field, field, P(None, None, "gz"), P("grp"), P(), P("grp"))
    return jax.shard_map(
        body, mesh=mesh, in_specs=placed, out_specs=(field, field, field), check_vma=False
    )
```

```python
import functools
import math

import jax
import jax.numpy as jnp
from jax import lax
from jax.experimental import pallas as pl
from jax.experimental.pallas import tpu as pltpu
from jax.sharding import PartitionSpec as P

ITERS = 4
SMAX = 4
COURANT = 0.6
MESH = pl.DeviceIdType.MESH

LANE = 128
PAD = 5
CHUNK = 4
REACH = ITERS * SMAX
FIRST_HOP, LAST_HOP = 3, 6
HANDED = 6
EARLY = 3


def kernel(
    rows,
    own,
    span,
    shifts_in,
    seq_in,
    eps_in,
    e_in,
    hx_in,
    hz_in,
    map_in,
    e_out,
    hx_out,
    hz_out,
    e0,
    hx0,
    hz0,
    e1,
    hx1,
    hz1,
    e2,
    hx2,
    hz2,
    e3,
    hx3,
    hz3,
    e4,
    hx4,
    hz4,
    coeff,
    design_rows,
    edge_rows,
    bound_out,
    bound_in,
    shifts_ref,
    seq_ref,
    eps_ref,
    scalar_sem,
    local_sem,
    edge_send,
    edge_recv,
    send_sem,
    recv_sem,
    bound_send_sem,
    bound_recv_sem,
    relay_send,
    relay_recv,
    stage_e,
    stage_hx,
    stage_hz,
    stage_bound,
    stage_recv,
    stage_bound_recv,
    forward_send,
    forward_bound_send,
    ahead_sem,
):
    me = lax.axis_index("gx")
    core = lax.axis_index("gz")
    count = lax.axis_size("gx")
    left = lax.rem(me + count - 1, count)
    right = lax.rem(me + 1, count)
    total = rows + REACH
    bands = total // 8
    own_bands = rows // 8
    chunks = own // CHUNK
    cells = own * LANE
    is_last = me == count - 1

    to_left = {"gx": left}
    to_right = {"gx": right}
    to_partner = {"gz": 1 - core}

    ins = (e_in, hx_in, hz_in)
    state = ((e0, hx0, hz0), (e1, hx1, hz1), (e2, hx2, hz2), (e3, hx3, hz3), (e4, hx4, hz4))
    start = state[0]
    mine = pl.ds(PAD * LANE, cells)

    def at(tile):
        return pl.ds(pl.multiple_of(tile * LANE, LANE), LANE)

    phase = lax.rem(me * rows, span)
    high = lax.rem(me * rows + rows, span)
    loads = [
        pltpu.make_async_copy(ins[f], start[f].at[pl.ds(0, rows), mine], local_sem.at[f])
        for f in range(3)
    ]
    loads.append(
        pltpu.make_async_copy(
            map_in.at[:, pl.ds(pl.multiple_of(phase, 8), rows), :],
            design_rows.at[:, pl.ds(0, rows), :],
            local_sem.at[3],
        )
    )
    loads.append(
        pltpu.make_async_copy(
            map_in.at[:, pl.ds(pl.multiple_of(high, 8), REACH), :],
            design_rows.at[:, pl.ds(rows, REACH), :],
            local_sem.at[4],
        )
    )
    scalars = [
        pltpu.make_async_copy(source, target, scalar_sem.at[k])
        for k, (source, target) in enumerate(
            ((shifts_in, shifts_ref), (seq_in, seq_ref), (eps_in, eps_ref))
        )
    ]
    for copy in scalars + loads:
        copy.start()

    side = math.isqrt(count)
    place = lax.rem(me, side)
    sends = me > 0
    receives = me < count - 1
    through = (me == 1) & (core == 0)
    direct = sends & ~through
    crossing = sends & (place == 0)
    hop_start = (me == 0) & (core == 1)
    hop_first = (me >= side) & (place == FIRST_HOP)
    hop_last = (me >= side) & (place == LAST_HOP)
    stage_target = {
        "gx": jnp.where(me == 1, 0, me + FIRST_HOP),
        "gz": jnp.where(me == 1, 1, core),
    }
    next_target = {"gx": me + (LAST_HOP - FIRST_HOP)}
    last_target = {
        "gx": jnp.where(me == 0, 0, me - LAST_HOP - 1),
        "gz": jnp.where(me == 0, 0, core),
    }
    flow_core = jnp.where(me == 0, 0, core)

    barrier = pltpu.get_barrier_semaphore()

    def greet(condition, target):
        @pl.when(condition)
        def _():
            pl.semaphore_signal(barrier, inc=1, device_id=target, device_id_type=MESH)

    greet(receives & (me > 0), to_right)
    greet(hop_start, {"gx": 1, "gz": 0})
    greet(hop_start, {"gx": 1, "gz": 1})
    greet(hop_first, {"gx": me - FIRST_HOP})
    row_end = (me >= side) & (place == side - 1)
    greet(receives & (place == side - 1), {"gx": me + side})
    pl.semaphore_signal(barrier, inc=1, device_id=to_partner, device_id_type=MESH)

    def gain_bands(which, own_tiles, edge_tile):
        gains = [COURANT * (1.0 / jnp.full((8, LANE), eps_ref[k], jnp.float32)) for k in range(4)]
        periods = (me * rows // span, (me * rows + rows) // span)
        designs = [jnp.full((8, LANE), seq_ref[p], jnp.int32) for p in periods]

        def gain_tile(source, r, tile, target):
            design = designs[0] if r < own_bands else designs[1]
            maps = [source[k, pl.ds(8 * r, 8), at(tile)] for k in range(source.shape[0])]
            level = maps[0]
            for k in range(1, len(maps)):
                level = jnp.where(design == k, maps[k], level)
            coeff[pl.ds(8 * r, 8), at(target)] = jnp.where(
                level < 2,
                jnp.where(level == 0, gains[0], gains[1]),
                jnp.where(level == 2, gains[2], gains[3]),
            )

        def one_tile(tile, carry):
            for r in which:
                gain_tile(design_rows, r, tile, tile + PAD)
            return carry

        if own_tiles:
            lax.fori_loop(0, own, one_tile, 0, unroll=2)
        if edge_tile:
            for r in which:
                gain_tile(edge_rows, r, 0, here)

    here = jnp.where(core == 0, PAD + own, PAD - 1)

    @pl.when(hop_start)
    def _():
        for copy in scalars + loads:
            copy.wait()
        gain_bands(range(bands), True, False)

    for condition, amount in (
        (~sends, 1),
        (sends & ~(crossing | row_end), 2),
        (crossing | row_end, 3),
    ):

        @pl.when(condition)
        def _(amount=amount):
            pl.semaphore_wait(barrier, amount)

    def tell(condition):
        @pl.when(condition)
        def _():
            pl.semaphore_signal(ahead_sem, inc=1, device_id=to_left, device_id_type=MESH)

    tell(hop_last | row_end)

    edge = (1 - core) * (own - 1)
    halo = jnp.where(core == 1, PAD + own, PAD - 1)
    outside = jnp.where(core == 1, PAD + own, PAD - 1)

    def remote(src, dst, send, recv, target):
        return pltpu.make_async_remote_copy(
            src_ref=src, dst_ref=dst, send_sem=send, recv_sem=recv, device_id=target, device_id_type=MESH
        )

    stages = (stage_e, stage_hx, stage_hz)

    def columns(flow, slot, shift):
        if isinstance(slot, int) and slot == chunks:
            first, tiles = (1 - flow) * (own - 1), 1
        else:
            tiles = CHUNK - 1 if isinstance(slot, int) and slot == chunks - 1 else CHUNK
            first = flow + slot * CHUNK
        return pl.ds(pl.multiple_of((first + shift) * LANE, LANE), tiles * LANE)

    def piece(f, slot, kind, handed=False):
        flow = flow_core if handed else core
        here_at = columns(flow, slot, 0)
        source = stages[f].at[:, here_at] if handed else ins[f].at[pl.ds(0, REACH), here_at]
        if kind == "direct":
            target = start[f].at[pl.ds(rows, REACH), columns(flow, slot, PAD)]
            device = last_target if handed else to_left
            arrived = recv_sem
        else:
            target = stages[f].at[:, here_at]
            device = next_target if handed else stage_target
            arrived = stage_recv
        sent = forward_send if handed else send_sem
        return remote(source, target, sent.at[f, slot], arrived.at[f, slot], device)

    def bound_piece(kind, handed=False):
        source = stage_bound if handed else bound_out.at[:, mine]
        sent = forward_bound_send if handed else bound_send_sem
        if kind == "direct":
            device = last_target if handed else to_left
            return remote(source, bound_in.at[:, mine], sent, bound_recv_sem, device)
        device = next_target if handed else stage_target
        return remote(source, stage_bound, sent, stage_bound_recv, device)

    def send(slots, bound=False):
        if bound:
            for condition, kind in ((direct, "direct"), (through, "stage")):

                @pl.when(condition)
                def _(kind=kind):
                    bound_piece(kind).start()

        for slot in slots:
            whole = slot == chunks or slot < HANDED
            for condition, kind in (
                (direct if whole else direct & ~crossing, "direct"),
                (through, "stage"),
            ):

                @pl.when(condition)
                def _(kind=kind, slot=slot):
                    for f in range(3):
                        piece(f, slot, kind).start()

    def hand_on(condition, kind, slots, bound=False):
        @pl.when(condition)
        def _():
            for slot in slots:
                for f in range(3):
                    piece(f, slot, "stage", True).wait_recv()
                    piece(f, slot, kind, True).start()
            if bound:
                bound_piece("stage", True).wait_recv()
                bound_piece(kind, True).start()

    partner_copies = [
        remote(
            ins[f].at[:, at(edge)],
            start[f].at[pl.ds(0, rows), at(halo)],
            edge_send.at[f],
            edge_recv.at[f],
            to_partner,
        )
        for f in range(3)
    ]
    partner_copies.append(
        remote(
            map_in.at[:, pl.ds(pl.multiple_of(phase, 8), rows), at(edge)],
            edge_rows.at[:, pl.ds(0, rows), :],
            edge_send.at[3],
            edge_recv.at[3],
            to_partner,
        )
    )
    partner_copies.append(
        remote(
            map_in.at[:, pl.ds(pl.multiple_of(high, 8), REACH), at(edge)],
            edge_rows.at[:, pl.ds(rows, REACH), :],
            edge_send.at[4],
            edge_recv.at[4],
            to_partner,
        )
    )
    for copy in partner_copies:
        copy.start()
    @pl.when(crossing)
    def _():
        for slot in range(HANDED, chunks):
            for f in range(3):
                piece(f, slot, "stage").start()

    send([chunks] + list(range(EARLY)))

    relays = [
        remote(
            start[f].at[pl.ds(rows, REACH), at(edge + PAD)],
            start[f].at[pl.ds(rows, REACH), at(halo)],
            relay_send.at[f],
            relay_recv.at[f],
            to_partner,
        )
        for f in range(3)
    ]
    relays.append(
        remote(
            bound_in.at[:, at(edge + PAD)],
            bound_in.at[:, at(halo)],
            relay_send.at[3],
            relay_recv.at[3],
            to_partner,
        )
    )

    def pass_edge(condition):
        @pl.when(condition)
        def _():
            for f in range(3):
                piece(f, chunks, "direct").wait_recv()
                relays[f].start()
            bound_piece("direct").wait_recv()
            relays[3].start()

    pass_edge(hop_start)
    hand_on(hop_start, "direct", [chunks] + list(range(EARLY)), bound=True)
    between = (me >= side) & (place > FIRST_HOP) & (place < LAST_HOP)

    @pl.when(between)
    def _():
        pl.semaphore_wait(ahead_sem, 1)

    tell(between)

    @pl.when(~hop_start)
    def _():
        for copy in scalars:
            copy.wait()

    lane = lax.broadcasted_iota(jnp.int32, (8, LANE), 1)
    sub = lax.broadcasted_iota(jnp.int32, (8, LANE), 0)
    zero = jnp.zeros((8, LANE), jnp.float32)
    last_vec = jnp.full((8, LANE), me, jnp.int32) == count - 1
    offsets = []
    offset = jnp.int32(0)
    for step in range(ITERS):
        offset = offset + shifts_ref[step]
        offsets.append(offset)

    for f in range(3):
        for r in range(bands):
            start[f][pl.ds(8 * r, 8), at(outside)] = zero

    def load(ref, r, tile):
        return ref[pl.ds(8 * r, 8), at(tile)]

    def advance(j, s, which, main):
        old, new = state[s - 1], state[s]
        base = CHUNK * j + PAD - s
        ahead_tiles = [[load(old[0], r, base + i) for r in which] for i in range(CHUNK + 1)]
        if main and s == 1:
            ahead_tiles = [
                [jnp.where(last_vec, 0.0, v) if r >= own_bands else v for r, v in zip(which, tile)]
                for tile in ahead_tiles
            ]
        hx_low = [load(new[1], r, base - 1) for r in which]
        cut_low = jnp.full((8, LANE), core * 1024 + j, jnp.int32) == 0
        cut_high = jnp.full((8, LANE), (1 - core) * 1024 + chunks - j, jnp.int32) == 0
        for i in range(CHUNK):
            tile = base + i
            e_now, e_right = ahead_tiles[i], ahead_tiles[i + 1]
            hx_new, hz_new = [], []
            bound = None
            if main:
                row = bound_in[pl.ds(s - 1, 1), at(tile)]
                bound = jnp.where(last_vec, 0.0, jnp.broadcast_to(row, (8, LANE)))
            for k, r in enumerate(which):
                e = e_now[k]
                hx = load(old[1], r, tile)
                hz = load(old[2], r, tile)
                if main and s == 1 and r >= own_bands:
                    hx = jnp.where(last_vec, 0.0, hx)
                    hz = jnp.where(last_vec, 0.0, hz)
                upper = pltpu.roll(jnp.where(lane == 0, e_right[k], e), LANE - 1, 1)
                hx = hx + COURANT * (upper - e)
                following = e_now[k + 1] if k + 1 < len(which) else (bound if main else zero)
                beyond = pltpu.roll(jnp.where(sub == 0, following, e), 7, 0)
                hz = hz - COURANT * (beyond - e)
                if i == s - 1:
                    hx = jnp.where(cut_low, 0.0, hx)
                if main and r < REACH // 8:
                    inside = sub + (me * rows + 8 * r) >= offsets[s - 1]
                    hz = jnp.where(inside, hz, 0.0)
                if main and r >= own_bands:
                    inside = sub + (me * rows + 8 * r) < offsets[s - 1] + count * rows
                    hx = jnp.where(inside, hx, 0.0)
                    hz = jnp.where(inside, hz, 0.0)
                hx_new.append(hx)
                hz_new.append(hz)
            for k, r in enumerate(which):
                e, hx, hz = e_now[k], hx_new[k], hz_new[k]
                lower = pltpu.roll(jnp.where(lane == LANE - 1, hx_low[k], hx), 1, 1)
                before = hz_new[k - 1] if k > 0 else zero
                behind = pltpu.roll(jnp.where(sub == 7, before, hz), 1, 0)
                e = e + load(coeff, r, tile) * ((hx - lower) - (hz - behind))
                if i == s:
                    e = jnp.where(cut_high, 0.0, e)
                if main and r >= own_bands:
                    inside = sub + (me * rows + 8 * r) < offsets[s - 1] + count * rows
                    e = jnp.where(inside, e, 0.0)
                new[0][pl.ds(8 * r, 8), at(tile)] = e
                new[1][pl.ds(8 * r, 8), at(tile)] = hx
                new[2][pl.ds(8 * r, 8), at(tile)] = hz
                if not main and r == REACH // 8:
                    bound_out[pl.ds(s, 1), at(tile)] = e[0:1]
                    if s == 1:
                        bound_out[pl.ds(0, 1), at(tile)] = e_now[k][0:1]
            hx_low = hx_new

    strip = [REACH // 8 - 1, REACH // 8]
    @pl.when(~hop_start)
    def _():
        for copy in loads:
            copy.wait()

    for copy in partner_copies:
        copy.wait_recv()
    gain_bands(range(bands), False, True)

    def strip_chunk(j, carry):
        for s in range(1, ITERS):
            advance(j, s, strip, False)
        return carry

    @pl.when(sends)
    def _():
        gain_bands(strip, True, False)
        lax.fori_loop(0, chunks + 1, strip_chunk, 0)
        gain_bands([r for r in range(bands) if r not in strip], True, False)

    at_start = (me == 0) & (core == 0)

    @pl.when(at_start)
    def _():
        gain_bands(range(bands), True, False)

    send(range(EARLY, chunks), bound=True)

    @pl.when(hop_first | hop_last)
    def _():
        pl.semaphore_wait(ahead_sem, 1)


    pass_edge(receives & (me > 0))

    @pl.when(at_start)
    def _():
        for f in range(3):
            piece(f, chunks, "direct").wait_recv()
        bound_piece("direct").wait_recv()

    @pl.when(receives)
    def _():
        @pl.when(~hop_start)
        def _():
            for copy in relays:
                copy.wait_recv()

        @pl.when(hop_start)
        def _():
            theirs = columns(0, chunks, 0)
            copies = [
                pltpu.make_async_copy(
                    stages[f].at[:, theirs], start[f].at[pl.ds(rows, REACH), at(here)], local_sem.at[f]
                )
                for f in range(3)
            ]
            copies.append(
                pltpu.make_async_copy(
                    stage_bound.at[:, theirs], bound_in.at[:, at(here)], local_sem.at[3]
                )
            )
            for copy in copies:
                copy.start()
            for copy in copies:
                copy.wait()

    moved = offsets[-1]
    turn = jnp.bitwise_and(moved, 7)
    back = jnp.bitwise_and(8 - turn, 7)
    moved_vec = jnp.full((8, LANE), moved, jnp.int32)
    turned = sub < jnp.full((8, LANE), turn, jnp.int32)
    everything = list(range(bands))
    outs = (e_out, hx_out, hz_out)

    def finish(j):
        for i in range(CHUNK):
            tile = CHUNK * j + PAD - ITERS + i
            for f in range(3):
                lines = [load(state[ITERS][f], r, tile) for r in range(bands)]
                for k in range(1, REACH // 8 + 1):
                    lines = [
                        jnp.where(moved_vec >= 8 * k, lines[r + 1], lines[r]) if r + 1 < bands else lines[r]
                        for r in range(bands)
                    ]
                for r in range(own_bands):
                    joined = jnp.where(turned, lines[r + 1], lines[r])
                    outs[f][pl.ds(8 * r, 8), at(tile - PAD)] = pltpu.roll(joined, back, 0)

    def main_chunk(j):
        for s in range(1, ITERS + 1):
            advance(j, s, everything, True)

    def arrive(j):
        @pl.when(receives)
        def _():
            for f in range(3):
                piece(f, j, "direct").wait_recv()

    def middle(j, carry):
        hand_on(hop_last & (j == EARLY), "direct", range(HANDED, chunks))
        hand_on(hop_start & (j >= EARLY), "direct", [j])
        arrive(j)
        main_chunk(j)
        finish(j)
        return carry

    hand_on(hop_first, "stage", range(HANDED, chunks))
    arrive(0)
    main_chunk(jnp.int32(0))
    lax.fori_loop(1, chunks - 1, middle, 0)
    hand_on(hop_start, "direct", [chunks - 1])
    arrive(chunks - 1)

    def closing(j, carry):
        main_chunk(j)
        finish(j)
        return carry

    lax.fori_loop(chunks - 1, chunks + 1, closing, 0)

    for copy in partner_copies:
        copy.wait_send()

    @pl.when(receives & ~at_start)
    def _():
        for copy in relays:
            copy.wait_send()

    def drain(condition, handed, slots, bound):
        @pl.when(condition)
        def _():
            if bound:
                bound_piece("direct", handed).wait_send()
            for slot in slots:
                for f in range(3):
                    piece(f, slot, "direct", handed).wait_send()

    drain(sends, False, range(chunks + 1), True)
    drain(hop_start, True, range(chunks + 1), True)
    drain(hop_first | hop_last, True, range(HANDED, chunks), False)


def store(e_in, hx_in, hz_in, e_out, hx_out, hz_out, sem):
    copies = [
        pltpu.make_async_copy(source, target, sem.at[k])
        for k, (source, target) in enumerate(
            ((e_in, e_out), (hx_in, hx_out), (hz_in, hz_out))
        )
    ]
    for copy in copies:
        copy.start()
    for copy in copies:
        copy.wait()


def body(electric, magnetic_x, magnetic_z, index_map, period_seq, eps_table, shifts):
    rows, cells = electric.shape
    own = cells // LANE
    width = (PAD + own + CHUNK) * LANE
    total = rows + REACH
    chunks = own // CHUNK
    types, span, _ = index_map.shape
    field = pltpu.VMEM((total, width), jnp.float32)
    dma = pltpu.SemaphoreType.DMA
    hbm = pl.BlockSpec(memory_space=pltpu.HBM)
    vmem = pl.BlockSpec(memory_space=pltpu.VMEM)
    out = jax.ShapeDtypeStruct((rows, cells), jnp.float32)
    fields = pl.pallas_call(
        functools.partial(kernel, rows, own, span),
        out_shape=(out, out, out),
        in_specs=[hbm] * 7,
        out_specs=(vmem, vmem, vmem),
        scratch_shapes=[field] * 16
        + [
            pltpu.VMEM((types, total, cells), jnp.int32),
            pltpu.VMEM((types, total, LANE), jnp.int32),
            pltpu.VMEM((ITERS, width), jnp.float32),
            pltpu.VMEM((ITERS, width), jnp.float32),
            pltpu.SMEM(shifts.shape, jnp.int32),
            pltpu.SMEM(period_seq.shape, jnp.int32),
            pltpu.SMEM(eps_table.shape, jnp.float32),
            dma((3,)),
            dma((5,)),
            dma((5,)),
            dma((5,)),
            dma((3, chunks + 1)),
            dma((3, chunks + 1)),
            dma,
            dma,
            dma((4,)),
            dma((4,)),
        ]
        + [pltpu.VMEM((REACH, cells), jnp.float32)] * 3
        + [
            pltpu.VMEM((ITERS, cells), jnp.float32),
            dma((3, chunks + 1)),
            dma,
            dma((3, chunks + 1)),
            dma,
            pltpu.SemaphoreType.REGULAR,
        ],
        compiler_params=pltpu.CompilerParams(
            collective_id=0, has_side_effects=True, vmem_limit_bytes=48 * 1024 * 1024
        ),
        name="yee",
    )(
        *(
            pltpu.with_memory_space_constraint(x, pltpu.HBM)
            for x in (shifts, period_seq, eps_table, electric, magnetic_x, magnetic_z, index_map)
        )
    )
    return pl.pallas_call(
        store,
        out_shape=(out, out, out),
        in_specs=[pl.BlockSpec(memory_space=pl.ANY)] * 3,
        out_specs=[hbm] * 3,
        scratch_shapes=[dma((3,))],
        compiler_params=pltpu.CompilerParams(vmem_limit_bytes=1024 * 1024),
        name="store",
    )(*fields)


def solution(mesh):
    field = P(("grp", "gx"), "gz")
    placed = (field, field, field, P(None, None, "gz"), P("grp"), P(), P("grp"))
    return jax.shard_map(
        body, mesh=mesh, in_specs=placed, out_specs=(field, field, field), check_vma=False
    )
```

```python
import functools
import math

import jax
import jax.numpy as jnp
from jax import lax
from jax.experimental import pallas as pl
from jax.experimental.pallas import tpu as pltpu
from jax.sharding import PartitionSpec as P

ITERS = 4
SMAX = 4
COURANT = 0.6
MESH = pl.DeviceIdType.MESH

LANE = 128
PAD = 5
CHUNK = 4
REACH = ITERS * SMAX
FIRST_HOP, LAST_HOP = 3, 6
HANDED = 6
EARLY = 3


def kernel(
    rows,
    own,
    span,
    shifts_in,
    seq_in,
    eps_in,
    e_in,
    hx_in,
    hz_in,
    map_in,
    e_out,
    hx_out,
    hz_out,
    e0,
    hx0,
    hz0,
    e1,
    hx1,
    hz1,
    e2,
    hx2,
    hz2,
    e3,
    hx3,
    hz3,
    e4,
    hx4,
    hz4,
    coeff,
    design_rows,
    edge_rows,
    bound_out,
    bound_in,
    shifts_ref,
    seq_ref,
    eps_ref,
    scalar_sem,
    local_sem,
    edge_send,
    edge_recv,
    send_sem,
    recv_sem,
    bound_send_sem,
    bound_recv_sem,
    relay_send,
    relay_recv,
    stage_e,
    stage_hx,
    stage_hz,
    stage_bound,
    stage_recv,
    stage_bound_recv,
    forward_send,
    forward_bound_send,
    ahead_sem,
):
    me = lax.axis_index("gx")
    core = lax.axis_index("gz")
    count = lax.axis_size("gx")
    left = lax.rem(me + count - 1, count)
    right = lax.rem(me + 1, count)
    total = rows + REACH
    bands = total // 8
    own_bands = rows // 8
    chunks = own // CHUNK
    cells = own * LANE
    is_last = me == count - 1

    to_left = {"gx": left}
    to_right = {"gx": right}
    to_partner = {"gz": 1 - core}

    ins = (e_in, hx_in, hz_in)
    state = ((e0, hx0, hz0), (e1, hx1, hz1), (e2, hx2, hz2), (e3, hx3, hz3), (e4, hx4, hz4))
    start = state[0]
    mine = pl.ds(PAD * LANE, cells)

    def at(tile):
        return pl.ds(pl.multiple_of(tile * LANE, LANE), LANE)

    phase = lax.rem(me * rows, span)
    high = lax.rem(me * rows + rows, span)
    loads = [
        pltpu.make_async_copy(ins[f], start[f].at[pl.ds(0, rows), mine], local_sem.at[f])
        for f in range(3)
    ]
    loads.append(
        pltpu.make_async_copy(
            map_in.at[:, pl.ds(pl.multiple_of(phase, 8), rows), :],
            design_rows.at[:, pl.ds(0, rows), :],
            local_sem.at[3],
        )
    )
    loads.append(
        pltpu.make_async_copy(
            map_in.at[:, pl.ds(pl.multiple_of(high, 8), REACH), :],
            design_rows.at[:, pl.ds(rows, REACH), :],
            local_sem.at[4],
        )
    )
    scalars = [
        pltpu.make_async_copy(source, target, scalar_sem.at[k])
        for k, (source, target) in enumerate(
            ((shifts_in, shifts_ref), (seq_in, seq_ref), (eps_in, eps_ref))
        )
    ]
    at_start = (me == 0) & (core == 0)
    for copy in scalars:
        copy.start()

    @pl.when(~at_start)
    def _():
        for copy in loads:
            copy.start()

    side = math.isqrt(count)
    place = lax.rem(me, side)
    sends = me > 0
    receives = me < count - 1
    through = (me == 1) & (core == 0)
    direct = sends & ~through
    crossing = sends & (place == 0)
    hop_start = (me == 0) & (core == 1)
    hop_first = (me >= side) & (place == FIRST_HOP)
    hop_last = (me >= side) & (place == LAST_HOP)
    stage_target = {
        "gx": jnp.where(me == 1, 0, me + FIRST_HOP),
        "gz": jnp.where(me == 1, 1, core),
    }
    next_target = {"gx": me + (LAST_HOP - FIRST_HOP)}
    last_target = {
        "gx": jnp.where(me == 0, 0, me - LAST_HOP - 1),
        "gz": jnp.where(me == 0, 0, core),
    }
    flow_core = jnp.where(me == 0, 0, core)

    barrier = pltpu.get_barrier_semaphore()

    def greet(condition, target):
        @pl.when(condition)
        def _():
            pl.semaphore_signal(barrier, inc=1, device_id=target, device_id_type=MESH)

    greet(receives & (me > 0), to_right)
    greet(hop_start, {"gx": 1, "gz": 0})
    greet(hop_start, {"gx": 1, "gz": 1})
    greet(hop_first, {"gx": me - FIRST_HOP})
    row_end = (me >= side) & (place == side - 1)
    greet(receives & (place == side - 1), {"gx": me + side})
    pl.semaphore_signal(barrier, inc=1, device_id=to_partner, device_id_type=MESH)

    def gain_bands(which, own_tiles, edge_tile):
        gains = [COURANT * (1.0 / jnp.full((8, LANE), eps_ref[k], jnp.float32)) for k in range(4)]
        periods = (me * rows // span, (me * rows + rows) // span)
        designs = [jnp.full((8, LANE), seq_ref[p], jnp.int32) for p in periods]

        def gain_tile(source, r, tile, target):
            design = designs[0] if r < own_bands else designs[1]
            maps = [source[k, pl.ds(8 * r, 8), at(tile)] for k in range(source.shape[0])]
            level = maps[0]
            for k in range(1, len(maps)):
                level = jnp.where(design == k, maps[k], level)
            coeff[pl.ds(8 * r, 8), at(target)] = jnp.where(
                level < 2,
                jnp.where(level == 0, gains[0], gains[1]),
                jnp.where(level == 2, gains[2], gains[3]),
            )

        def one_tile(tile, carry):
            for r in which:
                gain_tile(design_rows, r, tile, tile + PAD)
            return carry

        if own_tiles:
            lax.fori_loop(0, own, one_tile, 0, unroll=2)
        if edge_tile:
            for r in which:
                gain_tile(edge_rows, r, 0, here)

    here = jnp.where(core == 0, PAD + own, PAD - 1)

    @pl.when(hop_start)
    def _():
        for copy in scalars + loads:
            copy.wait()
        gain_bands(range(bands), True, False)

    for condition, amount in (
        (~sends, 1),
        (sends & ~(crossing | row_end), 2),
        (crossing | row_end, 3),
    ):

        @pl.when(condition)
        def _(amount=amount):
            pl.semaphore_wait(barrier, amount)

    def tell(condition):
        @pl.when(condition)
        def _():
            pl.semaphore_signal(ahead_sem, inc=1, device_id=to_left, device_id_type=MESH)

    tell(hop_last | row_end)

    edge = (1 - core) * (own - 1)
    halo = jnp.where(core == 1, PAD + own, PAD - 1)
    outside = jnp.where(core == 1, PAD + own, PAD - 1)

    def remote(src, dst, send, recv, target):
        return pltpu.make_async_remote_copy(
            src_ref=src, dst_ref=dst, send_sem=send, recv_sem=recv, device_id=target, device_id_type=MESH
        )

    stages = (stage_e, stage_hx, stage_hz)

    def columns(flow, slot, shift):
        if isinstance(slot, int) and slot == chunks:
            first, tiles = (1 - flow) * (own - 1), 1
        else:
            tiles = CHUNK - 1 if isinstance(slot, int) and slot == chunks - 1 else CHUNK
            first = flow + slot * CHUNK
        return pl.ds(pl.multiple_of((first + shift) * LANE, LANE), tiles * LANE)

    def piece(f, slot, kind, handed=False):
        flow = flow_core if handed else core
        here_at = columns(flow, slot, 0)
        source = stages[f].at[:, here_at] if handed else ins[f].at[pl.ds(0, REACH), here_at]
        if kind == "direct":
            target = start[f].at[pl.ds(rows, REACH), columns(flow, slot, PAD)]
            device = last_target if handed else to_left
            arrived = recv_sem
        else:
            target = stages[f].at[:, here_at]
            device = next_target if handed else stage_target
            arrived = stage_recv
        sent = forward_send if handed else send_sem
        return remote(source, target, sent.at[f, slot], arrived.at[f, slot], device)

    def bound_piece(kind, handed=False):
        source = stage_bound if handed else bound_out.at[:, mine]
        sent = forward_bound_send if handed else bound_send_sem
        if kind == "direct":
            device = last_target if handed else to_left
            return remote(source, bound_in.at[:, mine], sent, bound_recv_sem, device)
        device = next_target if handed else stage_target
        return remote(source, stage_bound, sent, stage_bound_recv, device)

    def send(slots, bound=False):
        if bound:
            for condition, kind in ((direct, "direct"), (through, "stage")):

                @pl.when(condition)
                def _(kind=kind):
                    bound_piece(kind).start()

        for slot in slots:
            whole = slot == chunks or slot < HANDED
            for condition, kind in (
                (direct if whole else direct & ~crossing, "direct"),
                (through, "stage"),
            ):

                @pl.when(condition)
                def _(kind=kind, slot=slot):
                    for f in range(3):
                        piece(f, slot, kind).start()

    def hand_on(condition, kind, slots, bound=False):
        @pl.when(condition)
        def _():
            for slot in slots:
                for f in range(3):
                    piece(f, slot, "stage", True).wait_recv()
                    piece(f, slot, kind, True).start()
            if bound:
                bound_piece("stage", True).wait_recv()
                bound_piece(kind, True).start()

    partner_copies = [
        remote(
            ins[f].at[:, at(edge)],
            start[f].at[pl.ds(0, rows), at(halo)],
            edge_send.at[f],
            edge_recv.at[f],
            to_partner,
        )
        for f in range(3)
    ]
    partner_copies.append(
        remote(
            map_in.at[:, pl.ds(pl.multiple_of(phase, 8), rows), at(edge)],
            edge_rows.at[:, pl.ds(0, rows), :],
            edge_send.at[3],
            edge_recv.at[3],
            to_partner,
        )
    )
    partner_copies.append(
        remote(
            map_in.at[:, pl.ds(pl.multiple_of(high, 8), REACH), at(edge)],
            edge_rows.at[:, pl.ds(rows, REACH), :],
            edge_send.at[4],
            edge_recv.at[4],
            to_partner,
        )
    )
    for copy in partner_copies:
        copy.start()

    @pl.when(at_start)
    def _():
        for copy in loads:
            copy.start()
    @pl.when(crossing)
    def _():
        for slot in range(HANDED, chunks):
            for f in range(3):
                piece(f, slot, "stage").start()

    send([chunks] + list(range(EARLY)))

    relays = [
        remote(
            start[f].at[pl.ds(rows, REACH), at(edge + PAD)],
            start[f].at[pl.ds(rows, REACH), at(halo)],
            relay_send.at[f],
            relay_recv.at[f],
            to_partner,
        )
        for f in range(3)
    ]
    relays.append(
        remote(
            bound_in.at[:, at(edge + PAD)],
            bound_in.at[:, at(halo)],
            relay_send.at[3],
            relay_recv.at[3],
            to_partner,
        )
    )

    def pass_edge(condition):
        @pl.when(condition)
        def _():
            for f in range(3):
                piece(f, chunks, "direct").wait_recv()
                relays[f].start()
            bound_piece("direct").wait_recv()
            relays[3].start()

    pass_edge(hop_start)
    hand_on(hop_start, "direct", [chunks] + list(range(EARLY)), bound=True)
    between = (me >= side) & (place > FIRST_HOP) & (place < LAST_HOP)

    @pl.when(between)
    def _():
        pl.semaphore_wait(ahead_sem, 1)

    tell(between)

    @pl.when(~hop_start)
    def _():
        for copy in scalars:
            copy.wait()

    lane = lax.broadcasted_iota(jnp.int32, (8, LANE), 1)
    sub = lax.broadcasted_iota(jnp.int32, (8, LANE), 0)
    zero = jnp.zeros((8, LANE), jnp.float32)
    last_vec = jnp.full((8, LANE), me, jnp.int32) == count - 1
    offsets = []
    offset = jnp.int32(0)
    for step in range(ITERS):
        offset = offset + shifts_ref[step]
        offsets.append(offset)

    for f in range(3):
        for r in range(bands):
            start[f][pl.ds(8 * r, 8), at(outside)] = zero

    def load(ref, r, tile):
        return ref[pl.ds(8 * r, 8), at(tile)]

    def advance(j, s, which, main):
        old, new = state[s - 1], state[s]
        base = CHUNK * j + PAD - s
        ahead_tiles = [[load(old[0], r, base + i) for r in which] for i in range(CHUNK + 1)]
        if main and s == 1:
            ahead_tiles = [
                [jnp.where(last_vec, 0.0, v) if r >= own_bands else v for r, v in zip(which, tile)]
                for tile in ahead_tiles
            ]
        hx_low = [load(new[1], r, base - 1) for r in which]
        cut_low = jnp.full((8, LANE), core * 1024 + j, jnp.int32) == 0
        cut_high = jnp.full((8, LANE), (1 - core) * 1024 + chunks - j, jnp.int32) == 0
        for i in range(CHUNK):
            tile = base + i
            e_now, e_right = ahead_tiles[i], ahead_tiles[i + 1]
            hx_new, hz_new = [], []
            bound = None
            if main:
                row = bound_in[pl.ds(s - 1, 1), at(tile)]
                bound = jnp.where(last_vec, 0.0, jnp.broadcast_to(row, (8, LANE)))
            for k, r in enumerate(which):
                e = e_now[k]
                hx = load(old[1], r, tile)
                hz = load(old[2], r, tile)
                if main and s == 1 and r >= own_bands:
                    hx = jnp.where(last_vec, 0.0, hx)
                    hz = jnp.where(last_vec, 0.0, hz)
                upper = pltpu.roll(jnp.where(lane == 0, e_right[k], e), LANE - 1, 1)
                hx = hx + COURANT * (upper - e)
                following = e_now[k + 1] if k + 1 < len(which) else (bound if main else zero)
                beyond = pltpu.roll(jnp.where(sub == 0, following, e), 7, 0)
                hz = hz - COURANT * (beyond - e)
                if i == s - 1:
                    hx = jnp.where(cut_low, 0.0, hx)
                if main and r < REACH // 8:
                    inside = sub + (me * rows + 8 * r) >= offsets[s - 1]
                    hz = jnp.where(inside, hz, 0.0)
                if main and r >= own_bands:
                    inside = sub + (me * rows + 8 * r) < offsets[s - 1] + count * rows
                    hx = jnp.where(inside, hx, 0.0)
                    hz = jnp.where(inside, hz, 0.0)
                hx_new.append(hx)
                hz_new.append(hz)
            for k, r in enumerate(which):
                e, hx, hz = e_now[k], hx_new[k], hz_new[k]
                lower = pltpu.roll(jnp.where(lane == LANE - 1, hx_low[k], hx), 1, 1)
                before = hz_new[k - 1] if k > 0 else zero
                behind = pltpu.roll(jnp.where(sub == 7, before, hz), 1, 0)
                e = e + load(coeff, r, tile) * ((hx - lower) - (hz - behind))
                if i == s:
                    e = jnp.where(cut_high, 0.0, e)
                if main and r >= own_bands:
                    inside = sub + (me * rows + 8 * r) < offsets[s - 1] + count * rows
                    e = jnp.where(inside, e, 0.0)
                new[0][pl.ds(8 * r, 8), at(tile)] = e
                new[1][pl.ds(8 * r, 8), at(tile)] = hx
                new[2][pl.ds(8 * r, 8), at(tile)] = hz
                if not main and r == REACH // 8:
                    bound_out[pl.ds(s, 1), at(tile)] = e[0:1]
                    if s == 1:
                        bound_out[pl.ds(0, 1), at(tile)] = e_now[k][0:1]
            hx_low = hx_new

    strip = [REACH // 8 - 1, REACH // 8]
    @pl.when(~hop_start)
    def _():
        for copy in loads:
            copy.wait()

    for copy in partner_copies:
        copy.wait_recv()
    gain_bands(range(bands), False, True)

    def strip_chunk(j, carry):
        for s in range(1, ITERS):
            advance(j, s, strip, False)
        return carry

    @pl.when(sends)
    def _():
        gain_bands(strip, True, False)
        lax.fori_loop(0, chunks + 1, strip_chunk, 0)
        gain_bands([r for r in range(bands) if r not in strip], True, False)

    @pl.when(at_start)
    def _():
        gain_bands(range(bands), True, False)

    send(range(EARLY, chunks), bound=True)

    @pl.when(hop_first | hop_last)
    def _():
        pl.semaphore_wait(ahead_sem, 1)


    pass_edge(receives & (me > 0))

    @pl.when(at_start)
    def _():
        for f in range(3):
            piece(f, chunks, "direct").wait_recv()
        bound_piece("direct").wait_recv()

    @pl.when(receives)
    def _():
        @pl.when(~hop_start)
        def _():
            for copy in relays:
                copy.wait_recv()

        @pl.when(hop_start)
        def _():
            theirs = columns(0, chunks, 0)
            copies = [
                pltpu.make_async_copy(
                    stages[f].at[:, theirs], start[f].at[pl.ds(rows, REACH), at(here)], local_sem.at[f]
                )
                for f in range(3)
            ]
            copies.append(
                pltpu.make_async_copy(
                    stage_bound.at[:, theirs], bound_in.at[:, at(here)], local_sem.at[3]
                )
            )
            for copy in copies:
                copy.start()
            for copy in copies:
                copy.wait()

    moved = offsets[-1]
    turn = jnp.bitwise_and(moved, 7)
    back = jnp.bitwise_and(8 - turn, 7)
    moved_vec = jnp.full((8, LANE), moved, jnp.int32)
    turned = sub < jnp.full((8, LANE), turn, jnp.int32)
    everything = list(range(bands))
    outs = (e_out, hx_out, hz_out)

    def finish(j):
        for i in range(CHUNK):
            tile = CHUNK * j + PAD - ITERS + i
            for f in range(3):
                lines = [load(state[ITERS][f], r, tile) for r in range(bands)]
                for k in range(1, REACH // 8 + 1):
                    lines = [
                        jnp.where(moved_vec >= 8 * k, lines[r + 1], lines[r]) if r + 1 < bands else lines[r]
                        for r in range(bands)
                    ]
                for r in range(own_bands):
                    joined = jnp.where(turned, lines[r + 1], lines[r])
                    outs[f][pl.ds(8 * r, 8), at(tile - PAD)] = pltpu.roll(joined, back, 0)

    def main_chunk(j):
        for s in range(1, ITERS + 1):
            advance(j, s, everything, True)

    def arrive(j):
        @pl.when(receives)
        def _():
            for f in range(3):
                piece(f, j, "direct").wait_recv()

    def middle(j, carry):
        hand_on(hop_last & (j == EARLY), "direct", range(HANDED, chunks))
        hand_on(hop_start & (j >= EARLY), "direct", [j])
        arrive(j)
        main_chunk(j)
        finish(j)
        return carry

    hand_on(hop_first, "stage", range(HANDED, chunks))
    arrive(0)
    main_chunk(jnp.int32(0))
    lax.fori_loop(1, chunks - 1, middle, 0)
    hand_on(hop_start, "direct", [chunks - 1])
    arrive(chunks - 1)

    def closing(j, carry):
        main_chunk(j)
        finish(j)
        return carry

    lax.fori_loop(chunks - 1, chunks + 1, closing, 0)

    for copy in partner_copies:
        copy.wait_send()

    @pl.when(receives & ~at_start)
    def _():
        for copy in relays:
            copy.wait_send()

    def drain(condition, handed, slots, bound):
        @pl.when(condition)
        def _():
            if bound:
                bound_piece("direct", handed).wait_send()
            for slot in slots:
                for f in range(3):
                    piece(f, slot, "direct", handed).wait_send()

    drain(sends, False, range(chunks + 1), True)
    drain(hop_start, True, range(chunks + 1), True)
    drain(hop_first | hop_last, True, range(HANDED, chunks), False)


def store(e_in, hx_in, hz_in, e_out, hx_out, hz_out, sem):
    copies = [
        pltpu.make_async_copy(source, target, sem.at[k])
        for k, (source, target) in enumerate(
            ((e_in, e_out), (hx_in, hx_out), (hz_in, hz_out))
        )
    ]
    for copy in copies:
        copy.start()
    for copy in copies:
        copy.wait()


def body(electric, magnetic_x, magnetic_z, index_map, period_seq, eps_table, shifts):
    rows, cells = electric.shape
    own = cells // LANE
    width = (PAD + own + CHUNK) * LANE
    total = rows + REACH
    chunks = own // CHUNK
    types, span, _ = index_map.shape
    field = pltpu.VMEM((total, width), jnp.float32)
    dma = pltpu.SemaphoreType.DMA
    hbm = pl.BlockSpec(memory_space=pltpu.HBM)
    vmem = pl.BlockSpec(memory_space=pltpu.VMEM)
    out = jax.ShapeDtypeStruct((rows, cells), jnp.float32)
    fields = pl.pallas_call(
        functools.partial(kernel, rows, own, span),
        out_shape=(out, out, out),
        in_specs=[hbm] * 7,
        out_specs=(vmem, vmem, vmem),
        scratch_shapes=[field] * 16
        + [
            pltpu.VMEM((types, total, cells), jnp.int32),
            pltpu.VMEM((types, total, LANE), jnp.int32),
            pltpu.VMEM((ITERS, width), jnp.float32),
            pltpu.VMEM((ITERS, width), jnp.float32),
            pltpu.SMEM(shifts.shape, jnp.int32),
            pltpu.SMEM(period_seq.shape, jnp.int32),
            pltpu.SMEM(eps_table.shape, jnp.float32),
            dma((3,)),
            dma((5,)),
            dma((5,)),
            dma((5,)),
            dma((3, chunks + 1)),
            dma((3, chunks + 1)),
            dma,
            dma,
            dma((4,)),
            dma((4,)),
        ]
        + [pltpu.VMEM((REACH, cells), jnp.float32)] * 3
        + [
            pltpu.VMEM((ITERS, cells), jnp.float32),
            dma((3, chunks + 1)),
            dma,
            dma((3, chunks + 1)),
            dma,
            pltpu.SemaphoreType.REGULAR,
        ],
        compiler_params=pltpu.CompilerParams(
            collective_id=0, has_side_effects=True, vmem_limit_bytes=48 * 1024 * 1024
        ),
        name="yee",
    )(
        *(
            pltpu.with_memory_space_constraint(x, pltpu.HBM)
            for x in (shifts, period_seq, eps_table, electric, magnetic_x, magnetic_z, index_map)
        )
    )
    return pl.pallas_call(
        store,
        out_shape=(out, out, out),
        in_specs=[pl.BlockSpec(memory_space=pl.ANY)] * 3,
        out_specs=[hbm] * 3,
        scratch_shapes=[dma((3,))],
        compiler_params=pltpu.CompilerParams(vmem_limit_bytes=1024 * 1024),
        name="store",
    )(*fields)


def solution(mesh):
    field = P(("grp", "gx"), "gz")
    placed = (field, field, field, P(None, None, "gz"), P("grp"), P(), P("grp"))
    return jax.shard_map(
        body, mesh=mesh, in_specs=placed, out_specs=(field, field, field), check_vma=False
    )
```
